32 devices in a mesh: slab: 16 (over z, x, core), grp: 2 (over y).
Axes of the slice: x: 2, y: 2, z: 4, core: 2. Of those that a mesh axis runs over, the one named last changes fastest.
Arguments:
- capture: float32 [2, 262144], P(None, ('slab', 'grp')), may hold values from -6 to 6
- dropped: int32 [16], P('slab'), may hold values from 0 to 8191
Outputs:
- max_held: float32 [128, 128, 128], P('slab', 'grp')
- coherent: float32 [2, 128, 128, 128], P(None, 'slab', 'grp')
The draws below stay inside these ranges and needn't reach their ends.
All inputs are finite; a program needn't handle non-finite values.
Results may differ from the reference program's by a relative error of at most 0.0001.
Values sent between devices are 32-bit elements; how exact they have to be, the bound alone decides.
A program may use at most 128 MiB of HBM per device.

```python
import math
import jax
import jax.numpy as jnp
from jax import lax

NCH = 256
HOP = 64
KW = 128
LW = 128
Q = 128
BLOCKS = 2
SAMPLES = 262144
N_SLAB = 16


def set_ends(values, own_key, smallest, top_value):
    shape = values.shape
    place = [jax.random.randint(jax.random.fold_in(own_key, axis), (), 0, shape[axis]) for axis in range(len(shape))]
    values = values.at[tuple(place)].set(smallest)
    longest = shape.index(max(shape))
    place[longest] = (place[longest] + 1) % shape[longest]
    return values.at[tuple(place)].set(top_value)


def steps_of(rng, extent, pieces, low, high):
    def one(position, parts):
        draws = jax.random.uniform(jax.random.fold_in(jax.random.fold_in(rng, 6), position), (parts,), jnp.float32, low / len(pieces), high / len(pieces))
        return jnp.repeat(jnp.exp(draws), extent[position] // parts).reshape((-1,) + (1,) * (len(extent) - position - 1))

    loudness = one(*pieces[0])
    for cut in pieces[1:]:
        loudness = loudness * one(*cut)
    return loudness


def gaussian(rng, dims, scale, bound, pieces=(), kind=jnp.bfloat16):
    loudness = steps_of(rng, dims, pieces, -0.22, 0.18) if pieces else 1.0
    array = jax.random.normal(rng, dims, jnp.float32) * scale * loudness
    return jnp.minimum(jnp.maximum(array, -bound), bound).astype(kind)


def setup_inputs(seed: int = 0) -> dict:
    streams_of = jax.random.split(jax.random.key(seed), 3)
    return {
        "capture": gaussian(streams_of[0], (2, SAMPLES), 1.0, 6.0, ((1, 32),), jnp.float32),
        "dropped": set_ends(jax.random.randint(streams_of[1], (N_SLAB,), 0, Q * HOP), jax.random.fold_in(streams_of[1], 1), 0, (Q * HOP) - 1).astype(jnp.int32),
    }


def reference(capture, dropped):
    lead_hops = NCH // HOP - 1
    slab_hops = BLOCKS * Q
    total_hops = N_SLAB * slab_hops
    padded = jnp.concatenate([jnp.zeros((2, lead_hops * HOP), capture.dtype), capture], axis=1)
    hop_rows = padded.reshape(2, total_hops + lead_hops, HOP)
    frames = jnp.concatenate([hop_rows[:, lag_index:lag_index + total_hops] for lag_index in range(lead_hops + 1)], axis=2)
    tap_index = jnp.arange(NCH, dtype=jnp.int32).astype(jnp.float32)
    window = 0.5 - 0.5 * jnp.cos(2.0 * math.pi * tap_index / NCH)
    scaling = 1.0 / jnp.sqrt(jnp.sum(window * window))
    signal = lax.complex(frames[0] * window, frames[1] * window)
    spectra = jnp.fft.fft(signal, axis=-1)[:, :KW + LW] * scaling
    stamps = jnp.arange(N_SLAB, dtype=jnp.int32) * (BLOCKS * Q * HOP) + jnp.cumsum(dropped).astype(jnp.int32)
    hop_start = jnp.arange(slab_hops, dtype=jnp.int32) * HOP
    clock_mod = ((stamps[:, None] % NCH + hop_start[None, :]) % NCH).reshape(total_hops)
    channels = jnp.arange(KW + LW, dtype=jnp.int32)
    chan_turns = (clock_mod[:, None] * channels[None, :] % NCH).astype(jnp.float32) * (2.0 * math.pi / NCH)
    shifted = spectra * lax.complex(jnp.cos(chan_turns), -jnp.sin(chan_turns))
    shifted = shifted.reshape(N_SLAB, BLOCKS, Q, KW + LW)
    clock_period = Q * HOP
    freq_bins = jnp.arange(Q, dtype=jnp.int32)
    cycle_turns = (freq_bins[None, :] * (stamps % clock_period)[:, None] % clock_period).astype(jnp.float32) * (2.0 * math.pi / clock_period)
    rotation = lax.complex(jnp.cos(cycle_turns), -jnp.sin(cycle_turns))

    def accumulate(state_pair, slab_item):
        largest, running = state_pair
        slab_spectra, slab_rotation = slab_item
        lower_bank = slab_spectra[:, :, :KW]
        upper_bank = slab_spectra[:, :, KW:]
        products = lower_bank[:, :, :, None] * jnp.conj(upper_bank)[:, :, None, :]
        surfaces = jnp.fft.fft(products, axis=1) / math.sqrt(Q)
        largest = jnp.maximum(largest, lax.optimization_barrier(jnp.max(jnp.abs(surfaces), axis=0)))
        running = running + slab_rotation[:, None, None] * lax.optimization_barrier(jnp.sum(surfaces, axis=0))
        return ((largest, running), None)
    empty_surface = jnp.zeros((Q, KW, LW), jnp.float32)
    (largest, running), unused = lax.scan(accumulate, (empty_surface, lax.complex(empty_surface, empty_surface)), (shifted, rotation))
    norm_scale = 1.0 / math.sqrt(N_SLAB * BLOCKS)
    coherent = jnp.stack([jnp.real(running), jnp.imag(running)]) * norm_scale
    return (largest, coherent)
```

```python
import functools
import math

import jax
import jax.numpy as jnp
import numpy as np
from jax import lax
from jax.experimental import pallas as pl
from jax.experimental.pallas import tpu as pltpu
from jax.sharding import PartitionSpec as P

NCH = 256
HOP = 64
KW = 128
LW = 128
Q = 128
BLOCKS = 2
LANES = 128


def split_np(table):
    hi = table.astype(jnp.bfloat16)
    lo = (table - hi.astype(np.float64)).astype(jnp.bfloat16)
    return jnp.asarray(hi), jnp.asarray(lo)


def split(values):
    hi = values.astype(jnp.bfloat16)
    lo = (values - hi.astype(jnp.float32)).astype(jnp.bfloat16)
    return hi, lo


def dft_tables():
    i = np.arange(NCH)
    w = 0.5 - 0.5 * np.cos(2.0 * np.pi * i / NCH)
    w = w / np.sqrt(np.sum(w * w))
    turns = (i[:, None] * i[None, :] % NCH) * (2.0 * np.pi / NCH)
    cos, sin = w[:, None] * np.cos(turns), w[:, None] * np.sin(turns)
    to_real = np.concatenate([cos, sin], 0)
    to_imag = np.concatenate([-sin, cos], 0)
    return to_real, to_imag


def dot3(a_hi, a_lo, b_hi, b_lo, dims):
    dot = functools.partial(
        lax.dot_general, dimension_numbers=(dims, ((), ())), preferred_element_type=jnp.float32
    )
    return dot(a_hi, b_hi) + dot(a_lo, b_hi) + dot(a_hi, b_lo)


def cos_turns(turns, period):
    v = (jnp.abs(turns.astype(jnp.float32) * (1.0 / period) - 0.5) - 0.25) * (2.0 * math.pi)
    v2 = v * v
    total = jnp.full_like(v, 1.0 / math.factorial(13))
    for order in (11, 9, 7, 5, 3, 1):
        sign = 1.0 if order % 4 == 1 else -1.0
        total = total * v2 + sign / math.factorial(order)
    return total * v


def rotation(turns, period):
    return cos_turns(turns & (period - 1), period), cos_turns((turns + period // 4) & (period - 1), period)


def flip(index, by, bits):
    total = 0
    for bit in range(bits):
        w = 2**bit
        total = total + ((index // w + by // w) % 2) * w
    return total


def surfaces(
    own_blk, own_info, ty_hi, ty_lo, txs, tx_hi, held, coh,
    buf, infos, acc, got, ends, *rest,
    slabs, groups, own_bins, own_w
):
    slots = rest[:4], rest[4:8]
    line_sem, x_sem, y_sem, diag_sem, recv_sem, isend_sem, irecv_sem, swap_sem = rest[8:]
    slab, grp = lax.axis_index("slab"), lax.axis_index("grp")
    bits = slabs.bit_length() - 1
    line = slabs // 4
    rows = Q // 2
    bins = 2 * own_bins
    pairs = bins // 2
    period = Q * HOP
    last = groups - 1
    zero = slab * 0
    core = slab % 2
    chip = (slab // 2) % 2
    level = slab // 4
    partner = (slab + 1 - 2 * core, grp)
    beside = (slab + 2 - 4 * chip, grp)
    across = (slab, 1 - grp)

    barrier = pltpu.get_barrier_semaphore()

    def peer(i):
        return (flip(slab, i // groups, bits), (grp + i) % groups)

    def greet(i, carry):
        pl.semaphore_signal(
            barrier, inc=1, device_id=peer(i), device_id_type=pl.DeviceIdType.MESH
        )
        return carry

    lax.fori_loop(1, slabs * groups, greet, 0)

    def at_step(i):
        return jnp.where(i <= level, level - i, i)

    def remote(src, dst, send, recv, target):
        return pltpu.make_async_remote_copy(
            src_ref=src, dst_ref=dst, send_sem=send, recv_sem=recv,
            device_id=target, device_id_type=pl.DeviceIdType.MESH,
        )

    def moved(z, dx, dg, send, target, own=False):
        place = 2 * z + (chip + dx) % 2
        g = (grp + dg) % groups
        src = own_blk if own else buf.at[place, g]
        return remote(src, buf.at[place, g], send, recv_sem.at[place, g], target)

    def arrived(z, dx, dg):
        moved(z, dx, dg, line_sem.at[0], partner).wait_recv()

    def info_copy(i):
        return remote(own_info, infos.at[slab], isend_sem.at[i], irecv_sem.at[slab], peer(i))

    def info_arrived(origin):
        remote(own_info, infos.at[origin], isend_sem.at[0], irecv_sem.at[origin], partner).wait_recv()

    def line_copy(i):
        z = at_step(i)
        return moved(level, 0, 0, line_sem.at[i], (slab + 4 * (z - level), grp), True)

    def to_x(i, own=False):
        return moved(at_step(i), 0, 0, x_sem.at[i], beside, own)

    def to_y(i, own=False):
        return moved(at_step(i), 0, 0, y_sem.at[i], across, own)

    def diagonal(i):
        odd = i % 2
        dx, dg = odd, 1 - odd
        return dx, dg

    def diagonal_y(i):
        return moved(at_step(i), 1, 0, diag_sem.at[i], across)

    def diagonal_x(i):
        return moved(at_step(i), 0, 1, diag_sem.at[i], beside)

    def from_line(i):
        arrived(at_step(i), 0, 0)
        to_x(i).start()
        to_y(i).start()

    def from_sides(i):
        z = at_step(i)

        @pl.when(z % 2 == 1)
        def _():
            arrived(z, 1, 0)
            diagonal_y(i).start()
            arrived(z, 0, 1)

        @pl.when(z % 2 == 0)
        def _():
            arrived(z, 0, 1)
            diagonal_x(i).start()
            arrived(z, 1, 0)

    def run(first, end, act):
        def body(i, carry):
            act(i)
            return carry

        lax.fori_loop(first, end, body, 0)

    def reach(i):
        z = at_step(i)
        down = i <= level
        first = 4 * z - jnp.where(down & (z > 0), 1, 0)
        end = 4 * z + jnp.where(down & (i > 0), 3, 4)

        def wait(m):
            @pl.when((m != slab) | (grp != last))
            def _():
                info_arrived(m)

        run(first, end, wait)
        before = jnp.where(down, z + 1, z - 1)
        summed = jnp.where(down, z + 1, z)
        total = jnp.zeros((4, LANES), jnp.float32)
        for k in range(4):
            total = total + infos[4 * jnp.where(i == 0, z, summed) + k, 4:8, :] * jnp.where(
                (i > 0) | (4 * z + k > slab - core), 1.0, 0.0
            )
        base = ends[jnp.where(i == 0, z, before)] * jnp.where(i == 0, 0.0, 1.0)
        ends[z] = base + jnp.concatenate([total, total], axis=0) * jnp.where(down & (i > 0), -1.0, 1.0)

    buf[slab // 2, grp] = own_blk[...]
    acc[...] = jnp.zeros_like(acc)
    ends[...] = jnp.zeros_like(ends)
    pl.semaphore_wait(barrier, slabs * groups - 1)

    to_x(0, True).start()
    to_y(0, True).start()
    run(1, line, lambda i: line_copy(i).start())

    @pl.when(grp == last)
    def _():
        infos[slab] = own_info[...]
        run(1, slabs * groups, lambda i: info_copy(i).start())

    lane = lax.broadcasted_iota(jnp.int32, (rows, LANES), 1)
    low = lane < HOP
    jlane = lax.broadcasted_iota(jnp.int32, (16, Q), 1)
    jlane = 2 * (jlane & (rows - 1)) + (jlane >= rows).astype(jnp.int32)
    turn = lax.broadcasted_iota(jnp.int32, (16, Q), 0)
    turn = jnp.where(turn < 8, 2 * turn + 1, 2 * bins * (slab // 2) + bins - 1)
    lanes8 = lax.broadcasted_iota(jnp.int32, (8, LANES), 1)
    lchan = KW + lanes8
    kchan = grp * own_w + (lanes8 & (own_w - 1))
    ksign = jnp.where(lanes8 < own_w, -1.0, 1.0)
    jsub = 2 * lax.broadcasted_iota(jnp.int32, (8, LANES), 0)

    def spread(array, count):
        return jnp.concatenate([array] * count, axis=0)

    def events(u):
        i = u // 4

        @pl.when((u % 4 == 0) & (i < line))
        def _():
            reach(i)

        @pl.when((u % 2 == 1) & (u >= 3) & ((u + 3) // 2 < line))
        def _():
            from_line((u + 3) // 2)

        @pl.when((u % 2 == 1) & (u >= 5) & ((u - 1) // 2 < line))
        def _():
            from_sides((u - 1) // 2)

        @pl.when((u % 4 == 2) & (i < line))
        def _():
            arrived(at_step(i), 1, 1)

    def prepare(u, slot):
        z = at_step(u // 4)
        g = u % 2
        dx = (u // 2) % 2
        n = 4 * z + 2 * ((chip + dx) % 2) + core
        place = n // 2
        before = jnp.maximum(n - 1, 0)
        a_hi, a_lo, w_hi, w_lo = slot
        rel = ends[z]
        for k in range(1, 4):
            drop = infos[4 * z + k, 4:8, :] * jnp.where(4 * z + k > n, 1.0, 0.0)
            rel = rel - jnp.concatenate([drop, drop], axis=0)
        stamp = rel.astype(jnp.int32)
        t = (spread(stamp, 2) + HOP * jlane) & (period - 1)
        phq = rotation((turn * t) & (2 * period - 1), 2 * period)
        phx = [rotation(kchan * ((stamp + HOP * (jsub + p)) & (NCH - 1)), NCH) for p in range(2)]
        phy = [rotation(lchan * ((stamp + HOP * (jsub + p)) & (NCH - 1)), NCH) for p in range(2)]

        from_info = jnp.where((g == 0) & (n > 0), 1.0, 0.0)
        from_blk = jnp.where(g == 0, 0.0, 1.0)
        even, odd = [], []
        for c in range(2):
            base = c * rows
            tail = infos[before, 2 * c : 2 * c + 2, :] * from_info
            tail = tail + buf[place, 0, base + rows - 2 : base + rows, :] * from_blk
            r0 = buf[place, g, base : base + rows, :]
            r1 = jnp.concatenate([tail[1:2], buf[place, g, base : base + rows - 1, :]], axis=0)
            r2 = jnp.concatenate([tail, buf[place, g, base : base + rows - 2, :]], axis=0)
            even += [
                pltpu.roll(jnp.where(low, r1, r2), HOP, 1),
                pltpu.roll(jnp.where(low, r0, r1), HOP, 1),
            ]
            odd += [r1, r0]
        f_hi, f_lo = [], []
        for part in (even, odd):
            hi, lo = split(jnp.concatenate(part, axis=1))
            f_hi.append(hi)
            f_lo.append(lo)
        f_hi = jnp.concatenate(f_hi, axis=0)
        f_lo = jnp.concatenate(f_lo, axis=0)
        dot = functools.partial(jnp.dot, preferred_element_type=jnp.float32)
        upper = dot3(f_hi, f_lo, ty_hi[...], ty_lo[...], ((1,), (0,)))
        twice = dot(f_hi, txs[grp])
        lower = twice[:, :LANES] + dot(f_lo, tx_hi[grp]) + twice[:, LANES:]

        zrs, zis, kxs = [], [], []
        for p in range(2):
            c, s = (spread(v, rows // 8) for v in phy[p])
            part = upper[p * rows : (p + 1) * rows]
            yr, yi = part[:, :LW], part[:, LW:]
            zrs.append(yr * c - yi * s)
            zis.append(yr * s + yi * c)
            c, s = spread(phx[p][0], rows // 8), spread(phx[p][1] * ksign, rows // 8)
            part = lower[p * rows : (p + 1) * rows]
            kxs.append(part * c + pltpu.roll(part, own_w, 1) * s)
        zr_hi, zr_lo = split(jnp.concatenate(zrs, axis=0))
        zi_hi, zi_lo = split(jnp.concatenate(zis, axis=0))

        def weights(zr, zi):
            return jnp.concatenate(
                [jnp.concatenate([zr, -zi], 1), jnp.concatenate([zi, zr], 1)], axis=0
            )

        w_hi[...] = weights(zr_hi, zi_hi)
        w_lo[...] = weights(zr_lo, zi_lo)
        x = jnp.concatenate(kxs, axis=0).T
        xr, xi = x[:own_w], x[own_w:]
        c, s = phq[0][8:9], phq[1][8:9]
        ur = xr * c - xi * s
        ui = xr * s + xi * c

        def put(q, real, imag):
            hi, lo = split(jnp.concatenate([real, imag], axis=1))
            a_hi[q * own_w : (q + 1) * own_w, :] = hi
            a_lo[q * own_w : (q + 1) * own_w, :] = lo

        for m in range(pairs):
            c, s = phq[0][m : m + 1], phq[1][m : m + 1]
            rc, rs, ic, is_ = ur * c, ur * s, ui * c, ui * s
            put(pairs + m, rc - is_, ic + rs)
            put(pairs - 1 - m, rc + is_, ic - rs)

    def accumulate(slot, half):
        a_hi, a_lo, w_hi, w_lo = slot
        count = own_bins * own_w
        at = half * count if isinstance(half, int) else pl.multiple_of(half * count, count)
        part = dot3(
            a_hi[pl.ds(at, count), :], a_lo[pl.ds(at, count), :], w_hi[...], w_lo[...], ((1,), (0,))
        )
        sr = part[:, :LW].reshape(own_bins, own_w, LW)
        si = part[:, LW:].reshape(own_bins, own_w, LW)
        acc[half, 0] = jnp.maximum(acc[half, 0], sr * sr + si * si)
        acc[half, 1] = acc[half, 1] + sr
        acc[half, 2] = acc[half, 2] + si

    def both(slot):
        accumulate(slot, 0)
        accumulate(slot, 1)

    units = 4 * line

    def pair(i, carry):
        u = 2 * i
        events(u + 1)
        prepare(u + 1, slots[1])
        both(slots[0])
        events(u + 2)
        prepare(u + 2, slots[0])
        both(slots[1])
        return carry

    reach(zero)
    from_sides(zero)
    if line > 1:
        from_line(zero + 1)
    prepare(zero, slots[0])
    if line > 2:
        from_line(zero + 2)
    if line > 1:
        from_sides(zero + 1)
    lax.fori_loop(0, units // 2 - 1, pair, 0)
    prepare(zero + units - 1, slots[1])
    swap = remote(acc.at[1 - core], got, swap_sem.at[0], swap_sem.at[1], partner)
    accumulate(slots[0], 1 - core)
    accumulate(slots[1], 1 - core)
    swap.start()
    accumulate(slots[0], core)
    accumulate(slots[1], core)

    total = jnp.zeros((4, LANES), jnp.float32)
    for k in range(4):
        total = total + infos[k, 4:8, :]
    stamp = (jnp.concatenate([total, total], axis=0) - ends[0]).astype(jnp.int32) & (period - 1)
    klane = lax.broadcasted_iota(jnp.int32, (own_w, LANES), 1)
    ksub = grp * own_w + lax.broadcasted_iota(jnp.int32, (own_w, LANES), 0)
    kl = rotation((ksub - KW - klane) * spread(stamp, own_w // 8), NCH)
    qrow = slab * own_bins + lax.broadcasted_iota(jnp.int32, (8, LANES), 0)
    ql = rotation(qrow * stamp, period)
    scale = 1.0 / math.sqrt(slabs * BLOCKS)
    swap.wait_recv()
    held[...] = jnp.sqrt(jnp.maximum(acc[core, 0], got[0]))
    for q in range(own_bins):
        c, s = ql[0][q : q + 1] * scale, ql[1][q : q + 1] * scale
        fc = kl[0] * c - kl[1] * s
        fs = kl[0] * s + kl[1] * c
        real = acc[core, 1, q] + got[1, q]
        imag = acc[core, 2, q] + got[2, q]
        coh[0, q] = real * fc - imag * fs
        coh[1, q] = real * fs + imag * fc

    @pl.when(grp == last)
    def _():
        run(1, slabs * groups, lambda i: info_copy(i).wait_send())

    run(1, line, lambda i: line_copy(i).wait_send())

    def sent(i):
        to_x(i).wait_send()
        to_y(i).wait_send()
        diagonal_x(i).wait_send()

    run(0, line, sent)
    swap.wait_send()


def on_device(capture, dropped):
    slabs = lax.axis_size("slab")
    groups = lax.axis_size("grp")
    own_bins = Q // slabs
    own_w = KW // groups
    local = capture.shape[1] // LANES
    to_real, to_imag = dft_tables()
    ty = np.concatenate([to_real[:, KW:], to_imag[:, KW:]], 1)
    tx = np.stack(
        [
            np.concatenate(
                [to_real[:, g * own_w : (g + 1) * own_w], to_imag[:, g * own_w : (g + 1) * own_w]], 1
            )
            for g in range(groups)
        ]
    ) / math.sqrt(Q)
    ty_hi, ty_lo = split_np(ty)
    tx_hi, tx_lo = split_np(tx)
    txs = jnp.concatenate([tx_hi, tx_lo], axis=2)
    blocks = capture.reshape(2 * local, LANES)
    tail = capture[:, capture.shape[1] - 2 * LANES :].reshape(4, LANES)
    drop = jnp.broadcast_to(dropped.astype(jnp.float32).reshape(1, 1), (4, LANES))
    info = jnp.concatenate([tail, drop], axis=0)
    dma = pltpu.SemaphoreType.DMA
    line = slabs // 4
    count = 2 * own_bins * own_w
    slot = [pltpu.VMEM((count, 2 * Q), jnp.bfloat16)] * 2
    slot = slot + [pltpu.VMEM((2 * Q, 2 * LW), jnp.bfloat16)] * 2
    held, coherent = pl.pallas_call(
        functools.partial(surfaces, slabs=slabs, groups=groups, own_bins=own_bins, own_w=own_w),
        out_shape=[
            jax.ShapeDtypeStruct((own_bins, own_w, LW), jnp.float32),
            jax.ShapeDtypeStruct((2, own_bins, own_w, LW), jnp.float32),
        ],
        in_specs=[pl.BlockSpec(memory_space=pltpu.VMEM)] * 6,
        out_specs=[pl.BlockSpec(memory_space=pltpu.VMEM)] * 2,
        scratch_shapes=[
            pltpu.VMEM((slabs // 2, groups, 2 * local, LANES), jnp.float32),
            pltpu.VMEM((slabs, 8, LANES), jnp.float32),
            pltpu.VMEM((2, 3, own_bins, own_w, LW), jnp.float32),
            pltpu.VMEM((3, own_bins, own_w, LW), jnp.float32),
            pltpu.VMEM((line, 8, LANES), jnp.float32),
            *slot,
            *slot,
            dma((line,)),
            dma((line,)),
            dma((line,)),
            dma((line,)),
            dma((slabs // 2, groups)),
            dma((slabs * groups,)),
            dma((slabs,)),
            dma((2,)),
        ],
        compiler_params=pltpu.CompilerParams(
            collective_id=0, has_side_effects=True, vmem_limit_bytes=48 * 2**20
        ),
    )(
        blocks,
        info,
        ty_hi, ty_lo, txs, tx_hi,
    )
    return held, coherent


def solution(mesh):
    in_specs = (P(None, ("slab", "grp")), P("slab"))
    out_specs = (P("slab", "grp", None), P(None, "slab", "grp", None))
    return jax.shard_map(
        on_device, mesh=mesh, in_specs=in_specs, out_specs=out_specs, check_vma=False
    )
```

```python
import functools
import math

import jax
import jax.numpy as jnp
import numpy as np
from jax import lax
from jax.experimental import pallas as pl
from jax.experimental.pallas import tpu as pltpu
from jax.sharding import PartitionSpec as P

NCH = 256
HOP = 64
KW = 128
LW = 128
Q = 128
BLOCKS = 2
LANES = 128


def split_np(table):
    hi = table.astype(jnp.bfloat16)
    lo = (table - hi.astype(np.float64)).astype(jnp.bfloat16)
    return jnp.asarray(hi), jnp.asarray(lo)


def split(values):
    hi = values.astype(jnp.bfloat16)
    lo = (values - hi.astype(jnp.float32)).astype(jnp.bfloat16)
    return hi, lo


def dft_tables():
    i = np.arange(NCH)
    w = 0.5 - 0.5 * np.cos(2.0 * np.pi * i / NCH)
    w = w / np.sqrt(np.sum(w * w))
    turns = (i[:, None] * i[None, :] % NCH) * (2.0 * np.pi / NCH)
    cos, sin = w[:, None] * np.cos(turns), w[:, None] * np.sin(turns)
    to_real = np.concatenate([cos, sin], 0)
    to_imag = np.concatenate([-sin, cos], 0)
    return to_real, to_imag


def dot3(a_hi, a_lo, b_hi, b_lo, dims):
    dot = functools.partial(
        lax.dot_general, dimension_numbers=(dims, ((), ())), preferred_element_type=jnp.float32
    )
    return dot(a_hi, b_hi) + dot(a_lo, b_hi) + dot(a_hi, b_lo)


def cos_turns(turns, period):
    v = (jnp.abs(turns.astype(jnp.float32) * (1.0 / period) - 0.5) - 0.25) * (2.0 * math.pi)
    v2 = v * v
    total = jnp.full_like(v, 1.0 / math.factorial(13))
    for order in (11, 9, 7, 5, 3, 1):
        sign = 1.0 if order % 4 == 1 else -1.0
        total = total * v2 + sign / math.factorial(order)
    return total * v


def rotation(turns, period):
    return cos_turns(turns & (period - 1), period), cos_turns((turns + period // 4) & (period - 1), period)


def surfaces(
    own_blk, own_info, ty_hbm, tx_hbm, held, coh,
    buf, infos, acc, got, ends, ty, txs, *rest,
    slabs, groups, own_bins, own_w
):
    slots = rest[:4], rest[4:8]
    line_sem, x_sem, y_sem, diag_sem, recv_sem, isend_sem, irecv_sem, swap_sem, load_sem = rest[8:]
    slab, grp = lax.axis_index("slab"), lax.axis_index("grp")
    bits = slabs.bit_length() - 1
    line = slabs // 4
    rows = Q // 2
    bins = 2 * own_bins
    pairs = bins // 2
    period = Q * HOP
    last = groups - 1
    zero = slab * 0
    core = slab % 2
    chip = (slab // 2) % 2
    level = slab // 4
    partner = (slab + 1 - 2 * core, grp)
    beside = (slab + 2 - 4 * chip, grp)
    across = (slab, 1 - grp)

    place = slab // 2

    def load(src, dst, i):
        return pltpu.make_async_copy(src, dst, load_sem.at[i])

    tables = [load(ty_hbm, ty, 0), load(tx_hbm.at[grp], txs, 1)]
    for copy in tables:
        copy.start()

    def chip_at(p):
        return (2 * p + core, grp)

    barrier = pltpu.get_barrier_semaphore()

    def greet(target):
        pl.semaphore_signal(barrier, inc=1, device_id=target, device_id_type=pl.DeviceIdType.MESH)

    def others(act):
        def body(i, carry):
            act((place + i) % (slabs // 2), i)
            return carry

        lax.fori_loop(1, slabs // 2, body, 0)

    greet(partner)
    greet(across)
    others(lambda p, i: greet(chip_at(p)))

    def at_step(i):
        return jnp.where(i <= level, level - i, i)

    def remote(src, dst, send, recv, target):
        return pltpu.make_async_remote_copy(
            src_ref=src, dst_ref=dst, send_sem=send, recv_sem=recv,
            device_id=target, device_id_type=pl.DeviceIdType.MESH,
        )

    def moved(z, dx, dg, send, target):
        at = 2 * z + (chip + dx) % 2
        g = (grp + dg) % groups
        return remote(buf.at[at, g], buf.at[at, g], send, recv_sem.at[at, g], target)

    def arrived(z, dx, dg):
        moved(z, dx, dg, line_sem.at[0], partner).wait_recv()

    def info_copy(first, count, send, recv, target):
        piece = infos.at[pl.ds(first, count)]
        return remote(piece, piece, isend_sem.at[send], irecv_sem.at[recv], target)

    chips = slabs // 2
    to_group = info_copy(slab, 1, 0, 0, across)
    to_partner = info_copy(slab, 1, chips, 1, partner)

    def to_chip(p, i):
        return info_copy(2 * place, 2, i, 2 + place, chip_at(p))

    def info_arrived(p):
        info_copy(2 * p, 2, 0, 2 + p, partner).wait_recv()

    def line_copy(i):
        return moved(level, 0, 0, line_sem.at[i], (slab + 4 * (at_step(i) - level), grp))

    def to_x(i):
        return moved(at_step(i), 0, 0, x_sem.at[i], beside)

    def to_y(i):
        return moved(at_step(i), 0, 0, y_sem.at[i], across)

    def diagonal_y(i):
        return moved(at_step(i), 1, 0, diag_sem.at[i], across)

    def diagonal_x(i):
        return moved(at_step(i), 0, 1, diag_sem.at[i], beside)

    def from_line(i):
        arrived(at_step(i), 0, 0)
        to_x(i).start()
        to_y(i).start()

    def from_sides(i):
        z = at_step(i)

        @pl.when(z % 2 == 1)
        def _():
            arrived(z, 1, 0)
            diagonal_y(i).start()
            arrived(z, 0, 1)

        @pl.when(z % 2 == 0)
        def _():
            arrived(z, 0, 1)
            diagonal_x(i).start()
            arrived(z, 1, 0)

    def run(first, end, act):
        def body(i, carry):
            act(i)
            return carry

        lax.fori_loop(first, end, body, 0)

    def reach(i):
        z = at_step(i)
        down = i <= level
        first = 2 * z - jnp.where(down & (z > 0), 1, 0)
        end = 2 * z + jnp.where(down & (i > 0), 1, 2)

        def wait(p):
            @pl.when(p != place)
            def _():
                info_arrived(p)

        run(first, end, wait)
        before = jnp.where(down, z + 1, z - 1)
        summed = jnp.where(down, z + 1, z)
        total = jnp.zeros((4, LANES), jnp.float32)
        for k in range(4):
            total = total + infos[4 * jnp.where(i == 0, z, summed) + k, 4:8, :] * jnp.where(
                (i > 0) | (4 * z + k > slab - core), 1.0, 0.0
            )
        base = ends[jnp.where(i == 0, z, before)] * jnp.where(i == 0, 0.0, 1.0)
        ends[z] = base + jnp.concatenate([total, total], axis=0) * jnp.where(down & (i > 0), -1.0, 1.0)

    own_load = load(own_blk, buf.at[place, grp], 2)
    info_load = load(own_info, infos.at[slab], 3)
    own_load.start()

    @pl.when(grp == last)
    def _():
        info_load.start()

    acc[...] = jnp.zeros_like(acc)
    ends[...] = jnp.zeros_like(ends)
    own_load.wait()

    @pl.when(grp == last)
    def _():
        info_load.wait()

    pl.semaphore_wait(barrier, chips + 1)

    @pl.when(grp == last)
    def _():
        to_group.start()
        to_partner.start()

    to_x(0).start()
    to_y(0).start()
    run(1, line, lambda i: line_copy(i).start())

    lane = lax.broadcasted_iota(jnp.int32, (rows, LANES), 1)
    low = lane < HOP
    jlane = lax.broadcasted_iota(jnp.int32, (16, Q), 1)
    jlane = 2 * (jlane & (rows - 1)) + (jlane >= rows).astype(jnp.int32)
    turn = lax.broadcasted_iota(jnp.int32, (16, Q), 0)
    turn = jnp.where(turn < 8, 2 * turn + 1, 2 * bins * (slab // 2) + bins - 1)
    lanes8 = lax.broadcasted_iota(jnp.int32, (8, LANES), 1)
    lchan = KW + lanes8
    kchan = grp * own_w + (lanes8 & (own_w - 1))
    ksign = jnp.where(lanes8 < own_w, -1.0, 1.0)
    jsub = 2 * lax.broadcasted_iota(jnp.int32, (8, LANES), 0)

    def spread(array, count):
        return jnp.concatenate([array] * count, axis=0)

    def events(u):
        i = u // 4

        @pl.when((u % 4 == 0) & (i < line))
        def _():
            reach(i)

        @pl.when((u % 2 == 1) & (u >= 3) & ((u + 3) // 2 < line))
        def _():
            from_line((u + 3) // 2)

        @pl.when((u % 2 == 1) & (u >= 5) & ((u - 1) // 2 < line))
        def _():
            from_sides((u - 1) // 2)

        @pl.when((u % 4 == 2) & (i < line))
        def _():
            arrived(at_step(i), 1, 1)

    def prepare(u, slot, first=False):
        z = at_step(u // 4)
        g = 1 - u % 2
        dx = (u // 2) % 2
        n = 4 * z + 2 * ((chip + dx) % 2) + core
        at = n // 2
        before = jnp.maximum(n - 1, 0)
        a_hi, a_lo, w_hi, w_lo = slot
        if first:
            rel = infos[slab, 4:8, :] * jnp.where(core > 0, 1.0, 0.0)
            rel = jnp.concatenate([rel, rel], axis=0)
        else:
            rel = ends[z]
            for k in range(1, 4):
                drop = infos[4 * z + k, 4:8, :] * jnp.where(4 * z + k > n, 1.0, 0.0)
                rel = rel - jnp.concatenate([drop, drop], axis=0)
        stamp = rel.astype(jnp.int32)
        t = (spread(stamp, 2) + HOP * jlane) & (period - 1)
        phq = rotation((turn * t) & (2 * period - 1), 2 * period)
        phx = [rotation(kchan * ((stamp + HOP * (jsub + p)) & (NCH - 1)), NCH) for p in range(2)]
        phy = [rotation(lchan * ((stamp + HOP * (jsub + p)) & (NCH - 1)), NCH) for p in range(2)]

        from_info = jnp.where((g == 0) & (n > 0), 1.0, 0.0)
        from_blk = jnp.where(g == 0, 0.0, 1.0)
        even, odd = [], []
        for c in range(2):
            base = c * rows
            tail = buf[at, 0, base + rows - 2 : base + rows, :]
            if not first:
                tail = tail * from_blk + infos[before, 2 * c : 2 * c + 2, :] * from_info
            r0 = buf[at, g, base : base + rows, :]
            r1 = jnp.concatenate([tail[1:2], buf[at, g, base : base + rows - 1, :]], axis=0)
            r2 = jnp.concatenate([tail, buf[at, g, base : base + rows - 2, :]], axis=0)
            even += [
                pltpu.roll(jnp.where(low, r1, r2), HOP, 1),
                pltpu.roll(jnp.where(low, r0, r1), HOP, 1),
            ]
            odd += [r1, r0]
        f_hi, f_lo = [], []
        for part in (even, odd):
            hi, lo = split(jnp.concatenate(part, axis=1))
            f_hi.append(hi)
            f_lo.append(lo)
        f_hi = jnp.concatenate(f_hi, axis=0)
        f_lo = jnp.concatenate(f_lo, axis=0)
        dot = functools.partial(jnp.dot, preferred_element_type=jnp.float32)
        upper = dot3(f_hi, f_lo, ty[0], ty[1], ((1,), (0,)))
        twice = dot(f_hi, txs[...])
        lower = twice[:, :LANES] + dot(f_lo, txs[:, :LANES]) + twice[:, LANES:]

        zrs, zis, kxs = [], [], []
        for p in range(2):
            c, s = (spread(v, rows // 8) for v in phy[p])
            part = upper[p * rows : (p + 1) * rows]
            yr, yi = part[:, :LW], part[:, LW:]
            zrs.append(yr * c - yi * s)
            zis.append(yr * s + yi * c)
            c, s = spread(phx[p][0], rows // 8), spread(phx[p][1] * ksign, rows // 8)
            part = lower[p * rows : (p + 1) * rows]
            kxs.append(part * c + pltpu.roll(part, own_w, 1) * s)
        zr_hi, zr_lo = split(jnp.concatenate(zrs, axis=0))
        zi_hi, zi_lo = split(jnp.concatenate(zis, axis=0))

        def weights(zr, zi):
            return jnp.concatenate(
                [jnp.concatenate([zr, -zi], 1), jnp.concatenate([zi, zr], 1)], axis=0
            )

        w_hi[...] = weights(zr_hi, zi_hi)
        w_lo[...] = weights(zr_lo, zi_lo)
        x = jnp.concatenate(kxs, axis=0).T
        xr, xi = x[:own_w], x[own_w:]
        c, s = phq[0][8:9], phq[1][8:9]
        ur = xr * c - xi * s
        ui = xr * s + xi * c

        def put(q, real, imag):
            hi, lo = split(jnp.concatenate([real, imag], axis=1))
            a_hi[q * own_w : (q + 1) * own_w, :] = hi
            a_lo[q * own_w : (q + 1) * own_w, :] = lo

        for m in range(pairs):
            c, s = phq[0][m : m + 1], phq[1][m : m + 1]
            rc, rs, ic, is_ = ur * c, ur * s, ui * c, ui * s
            put(pairs + m, rc - is_, ic + rs)
            put(pairs - 1 - m, rc + is_, ic - rs)

    def accumulate(slot, half):
        a_hi, a_lo, w_hi, w_lo = slot
        count = own_bins * own_w
        at = half * count if isinstance(half, int) else pl.multiple_of(half * count, count)
        part = dot3(
            a_hi[pl.ds(at, count), :], a_lo[pl.ds(at, count), :], w_hi[...], w_lo[...], ((1,), (0,))
        )
        sr = part[:, :LW].reshape(own_bins, own_w, LW)
        si = part[:, LW:].reshape(own_bins, own_w, LW)
        acc[half, 0] = jnp.maximum(acc[half, 0], sr * sr + si * si)
        acc[half, 1] = acc[half, 1] + sr
        acc[half, 2] = acc[half, 2] + si

    def both(slot):
        accumulate(slot, 0)
        accumulate(slot, 1)

    units = 4 * line

    def pair(i, carry):
        u = 2 * i
        events(u + 1)
        prepare(u + 1, slots[1])
        both(slots[0])
        events(u + 2)
        prepare(u + 2, slots[0])
        both(slots[1])
        return carry

    @pl.when(grp != last)
    def _():
        to_group.wait_recv()
        to_partner.start()

    info_copy(slab + 1 - 2 * core, 1, 0, 1, partner).wait_recv()
    others(lambda p, i: to_chip(p, i).start())
    for copy in tables:
        copy.wait()
    if line > 1:
        from_line(zero + 1)
    from_sides(zero)
    prepare(zero, slots[0], True)
    reach(zero)
    if line > 2:
        from_line(zero + 2)
    prepare(zero + 1, slots[1])
    accumulate(slots[0], 0)
    accumulate(slots[0], 1)
    arrived(at_step(zero), 1, 1)
    if line > 1:
        from_sides(zero + 1)
    prepare(zero + 2, slots[0])
    accumulate(slots[1], 0)
    accumulate(slots[1], 1)
    lax.fori_loop(1, units // 2 - 1, pair, 0)
    prepare(zero + units - 1, slots[1])
    swap = remote(acc.at[1 - core], got, swap_sem.at[0], swap_sem.at[1], partner)
    accumulate(slots[0], 1 - core)
    accumulate(slots[1], 1 - core)
    swap.start()
    accumulate(slots[0], core)
    accumulate(slots[1], core)

    total = jnp.zeros((4, LANES), jnp.float32)
    for k in range(4):
        total = total + infos[k, 4:8, :]
    stamp = (jnp.concatenate([total, total], axis=0) - ends[0]).astype(jnp.int32) & (period - 1)
    klane = lax.broadcasted_iota(jnp.int32, (own_w, LANES), 1)
    ksub = grp * own_w + lax.broadcasted_iota(jnp.int32, (own_w, LANES), 0)
    kl = rotation((ksub - KW - klane) * spread(stamp, own_w // 8), NCH)
    qrow = slab * own_bins + lax.broadcasted_iota(jnp.int32, (8, LANES), 0)
    ql = rotation(qrow * stamp, period)
    scale = 1.0 / math.sqrt(slabs * BLOCKS)
    swap.wait_recv()
    held[...] = jnp.sqrt(jnp.maximum(acc[core, 0], got[0]))
    for q in range(own_bins):
        c, s = ql[0][q : q + 1] * scale, ql[1][q : q + 1] * scale
        fc = kl[0] * c - kl[1] * s
        fs = kl[0] * s + kl[1] * c
        real = acc[core, 1, q] + got[1, q]
        imag = acc[core, 2, q] + got[2, q]
        coh[0, q] = real * fc - imag * fs
        coh[1, q] = real * fs + imag * fc

    @pl.when(grp == last)
    def _():
        to_group.wait_send()

    to_partner.wait_send()
    others(lambda p, i: to_chip(p, i).wait_send())
    run(1, line, lambda i: line_copy(i).wait_send())

    def sent(i):
        to_x(i).wait_send()
        to_y(i).wait_send()
        diagonal_x(i).wait_send()

    run(0, line, sent)
    swap.wait_send()


def on_device(capture, dropped):
    slabs = lax.axis_size("slab")
    groups = lax.axis_size("grp")
    own_bins = Q // slabs
    own_w = KW // groups
    local = capture.shape[1] // LANES
    to_real, to_imag = dft_tables()
    ty = np.concatenate([to_real[:, KW:], to_imag[:, KW:]], 1)
    tx = np.stack(
        [
            np.concatenate(
                [to_real[:, g * own_w : (g + 1) * own_w], to_imag[:, g * own_w : (g + 1) * own_w]], 1
            )
            for g in range(groups)
        ]
    ) / math.sqrt(Q)
    ty = jnp.stack(split_np(ty))
    txs = jnp.concatenate(split_np(tx), axis=2)
    blocks = capture.reshape(2 * local, LANES)
    tail = capture[:, capture.shape[1] - 2 * LANES :].reshape(4, LANES)
    drop = jnp.broadcast_to(dropped.astype(jnp.float32).reshape(1, 1), (4, LANES))
    info = jnp.concatenate([tail, drop], axis=0)
    dma = pltpu.SemaphoreType.DMA
    line = slabs // 4
    count = 2 * own_bins * own_w
    slot = [pltpu.VMEM((count, 2 * Q), jnp.bfloat16)] * 2
    slot = slot + [pltpu.VMEM((2 * Q, 2 * LW), jnp.bfloat16)] * 2
    held, coherent = pl.pallas_call(
        functools.partial(surfaces, slabs=slabs, groups=groups, own_bins=own_bins, own_w=own_w),
        out_shape=[
            jax.ShapeDtypeStruct((own_bins, own_w, LW), jnp.float32),
            jax.ShapeDtypeStruct((2, own_bins, own_w, LW), jnp.float32),
        ],
        in_specs=[pl.BlockSpec(memory_space=pltpu.HBM)] * 4,
        out_specs=[pl.BlockSpec(memory_space=pltpu.VMEM)] * 2,
        scratch_shapes=[
            pltpu.VMEM((slabs // 2, groups, 2 * local, LANES), jnp.float32),
            pltpu.VMEM((slabs, 8, LANES), jnp.float32),
            pltpu.VMEM((2, 3, own_bins, own_w, LW), jnp.float32),
            pltpu.VMEM((3, own_bins, own_w, LW), jnp.float32),
            pltpu.VMEM((line, 8, LANES), jnp.float32),
            pltpu.VMEM(ty.shape, jnp.bfloat16),
            pltpu.VMEM(txs.shape[1:], jnp.bfloat16),
            *slot,
            *slot,
            dma((line,)),
            dma((line,)),
            dma((line,)),
            dma((line,)),
            dma((slabs // 2, groups)),
            dma((slabs // 2 + 1,)),
            dma((slabs // 2 + 2,)),
            dma((2,)),
            dma((4,)),
        ],
        compiler_params=pltpu.CompilerParams(
            collective_id=0, has_side_effects=True, vmem_limit_bytes=48 * 2**20
        ),
    )(
        blocks,
        info,
        ty,
        txs,
    )
    return held, coherent


def solution(mesh):
    in_specs = (P(None, ("slab", "grp")), P("slab"))
    out_specs = (P("slab", "grp", None), P(None, "slab", "grp", None))
    return jax.shard_map(
        on_device, mesh=mesh, in_specs=in_specs, out_specs=out_specs, check_vma=False
    )
```

```python
import functools
import math

import jax
import jax.numpy as jnp
import numpy as np
from jax import lax
from jax.experimental import pallas as pl
from jax.experimental.pallas import tpu as pltpu
from jax.sharding import PartitionSpec as P

NCH = 256
HOP = 64
KW = 128
LW = 128
Q = 128
BLOCKS = 2
LANES = 128
VMEM_LIMIT = 67043328 - 1100 * 2**10


def split_np(table):
    hi = table.astype(jnp.bfloat16)
    lo = (table - hi.astype(np.float64)).astype(jnp.bfloat16)
    return jnp.asarray(hi), jnp.asarray(lo)


def split(values):
    hi = values.astype(jnp.bfloat16)
    lo = (values - hi.astype(jnp.float32)).astype(jnp.bfloat16)
    return hi, lo


def dft_tables():
    i = np.arange(NCH)
    w = 0.5 - 0.5 * np.cos(2.0 * np.pi * i / NCH)
    w = w / np.sqrt(np.sum(w * w))
    turns = (i[:, None] * i[None, :] % NCH) * (2.0 * np.pi / NCH)
    cos, sin = w[:, None] * np.cos(turns), w[:, None] * np.sin(turns)
    to_real = np.concatenate([cos, sin], 0)
    to_imag = np.concatenate([-sin, cos], 0)
    return to_real, to_imag


def dot3(a_hi, a_lo, b_hi, b_lo, dims):
    dot = functools.partial(
        lax.dot_general, dimension_numbers=(dims, ((), ())), preferred_element_type=jnp.float32
    )
    return dot(a_hi, b_hi) + dot(a_lo, b_hi) + dot(a_hi, b_lo)


def cos_turns(turns, period):
    v = (jnp.abs(turns.astype(jnp.float32) * (1.0 / period) - 0.5) - 0.25) * (2.0 * math.pi)
    v2 = v * v
    total = jnp.full_like(v, 1.0 / math.factorial(13))
    for order in (11, 9, 7, 5, 3, 1):
        sign = 1.0 if order % 4 == 1 else -1.0
        total = total * v2 + sign / math.factorial(order)
    return total * v


def rotation(turns, period):
    return cos_turns(turns & (period - 1), period), cos_turns((turns + period // 4) & (period - 1), period)

def surfaces(
    own_hbm, own_drop, ty_hbm, tx_hbm, held, coh,
    raw, buf, infos, acc, got, ends, ty, txs, *rest,
    slabs, groups, own_bins, own_w
):
    a_hi, a_lo, w_hi, w_lo, spec_y, spec_x = rest[:6]
    line_sem, x_sem, y_sem, diag_sem, recv_sem, isend_sem, irecv_sem, swap_sem, load_sem = rest[6:]
    slab, grp = lax.axis_index("slab"), lax.axis_index("grp")
    bits = slabs.bit_length() - 1
    line = slabs // 4
    rows = Q // 2
    bins = 2 * own_bins
    pairs = bins // 2
    cut = min(4, own_bins)
    cuts = own_bins // cut
    period = Q * HOP
    last = groups - 1
    zero = slab * 0
    core = slab % 2
    chip = (slab // 2) % 2
    level = slab // 4
    partner = (slab + 1 - 2 * core, grp)
    beside = (slab + 2 - 4 * chip, grp)
    across = (slab, 1 - grp)

    place = slab // 2

    def load(src, dst, i):
        return pltpu.make_async_copy(src, dst, load_sem.at[i])

    own_load = load(own_hbm, raw, 2)
    own_load.start()
    tables = [load(ty_hbm, ty, 0), load(tx_hbm.at[grp], txs, 1)]
    for copy in tables:
        copy.start()

    def chip_at(p):
        return (2 * p + core, grp)

    barrier = pltpu.get_barrier_semaphore()

    def greet(target):
        pl.semaphore_signal(barrier, inc=1, device_id=target, device_id_type=pl.DeviceIdType.MESH)

    def others(act):
        def body(i, carry):
            act((place + i) % (slabs // 2), i)
            return carry

        lax.fori_loop(1, slabs // 2, body, 0)

    greet(partner)
    greet(across)
    others(lambda p, i: greet(chip_at(p)))

    def at_step(i):
        return jnp.where(i <= level, level - i, i)

    def remote(src, dst, send, recv, target):
        return pltpu.make_async_remote_copy(
            src_ref=src, dst_ref=dst, send_sem=send, recv_sem=recv,
            device_id=target, device_id_type=pl.DeviceIdType.MESH,
        )

    def moved(z, dx, dg, send, target):
        at = 2 * z + (chip + dx) % 2
        g = (grp + dg) % groups
        return remote(buf.at[at, g], buf.at[at, g], send, recv_sem.at[at, g], target)

    def arrived(z, dx, dg):
        moved(z, dx, dg, line_sem.at[0], partner).wait_recv()

    def info_copy(first, count, send, recv, target):
        piece = infos.at[pl.ds(first, count)]
        return remote(piece, piece, isend_sem.at[send], irecv_sem.at[recv], target)

    chips = slabs // 2
    to_group = info_copy(slab, 1, 0, 0, across)
    to_partner = info_copy(slab, 1, chips, 1, partner)

    def to_chip(p, i):
        return info_copy(2 * place, 2, i, 2 + place, chip_at(p))

    def info_arrived(p):
        info_copy(2 * p, 2, 0, 2 + p, partner).wait_recv()

    def line_copy(i):
        return moved(level, 0, 0, line_sem.at[i], (slab + 4 * (at_step(i) - level), grp))

    def to_x(i):
        return moved(at_step(i), 0, 0, x_sem.at[i], beside)

    def to_y(i):
        return moved(at_step(i), 0, 0, y_sem.at[i], across)

    def diagonal_y(i):
        return moved(at_step(i), 1, 0, diag_sem.at[i], across)

    def diagonal_x(i):
        return moved(at_step(i), 0, 1, diag_sem.at[i], beside)

    def from_line(i):
        arrived(at_step(i), 0, 0)
        to_x(i).start()
        to_y(i).start()

    def from_sides(i):
        z = at_step(i)

        @pl.when(z % 2 == 1)
        def _():
            arrived(z, 1, 0)
            diagonal_y(i).start()
            arrived(z, 0, 1)

        @pl.when(z % 2 == 0)
        def _():
            arrived(z, 0, 1)
            diagonal_x(i).start()
            arrived(z, 1, 0)

    def run(first, end, act):
        def body(i, carry):
            act(i)
            return carry

        lax.fori_loop(first, end, body, 0)

    def reach(i):
        z = at_step(i)
        down = i <= level
        first = 2 * z - jnp.where(down & (z > 0), 1, 0)
        end = 2 * z + jnp.where(down & (i > 0), 1, 2)

        def wait(p):
            @pl.when(p != place)
            def _():
                info_arrived(p)

        run(first, end, wait)
        before = jnp.where(down, z + 1, z - 1)
        summed = jnp.where(down, z + 1, z)
        total = jnp.zeros((4, LANES), jnp.float32)
        for k in range(4):
            total = total + infos[4 * jnp.where(i == 0, z, summed) + k, 4:8, :] * jnp.where(
                (i > 0) | (4 * z + k > slab - core), 1.0, 0.0
            )
        base = ends[jnp.where(i == 0, z, before)] * jnp.where(i == 0, 0.0, 1.0)
        ends[z] = base + jnp.concatenate([total, total], axis=0) * jnp.where(down & (i > 0), -1.0, 1.0)

    ends[...] = jnp.zeros_like(ends)
    acc[...] = jnp.zeros_like(acc)
    own_load.wait()
    for c in range(2):
        buf[place, grp, c * rows : (c + 1) * rows, :] = raw[:, c, :]

    @pl.when(grp == last)
    def _():
        infos[slab] = jnp.concatenate(
            [
                raw[rows - 2 :, 0, :],
                raw[rows - 2 :, 1, :],
                jnp.broadcast_to(own_drop[0].astype(jnp.float32), (4, LANES)),
            ],
            axis=0,
        )

    pl.semaphore_wait(barrier, chips + 1)

    @pl.when(grp == last)
    def _():
        to_group.start()
        to_partner.start()

    to_x(0).start()
    to_y(0).start()
    run(1, line, lambda i: line_copy(i).start())

    lane = lax.broadcasted_iota(jnp.int32, (rows, LANES), 1)
    low = lane < HOP
    jlane = lax.broadcasted_iota(jnp.int32, (16, Q), 1)
    jlane = 2 * (jlane & (rows - 1)) + (jlane >= rows).astype(jnp.int32)
    turn = lax.broadcasted_iota(jnp.int32, (16, Q), 0)
    turn = jnp.where(turn < 8, 2 * turn + 1, 2 * bins * (slab // 2) + bins - 1)
    lanes8 = lax.broadcasted_iota(jnp.int32, (8, LANES), 1)
    lchan = KW + lanes8
    kchan = grp * own_w + (lanes8 & (own_w - 1))
    ksign = jnp.where(lanes8 < own_w, -1.0, 1.0)
    jsub = 2 * lax.broadcasted_iota(jnp.int32, (8, LANES), 0)

    def spread(array, count):
        return jnp.concatenate([array] * count, axis=0)

    def events(u):
        i = u // 4

        @pl.when((u % 4 == 0) & (i < line))
        def _():
            reach(i)

        @pl.when((u % 2 == 1) & (u >= 3) & ((u + 3) // 2 < line))
        def _():
            from_line((u + 3) // 2)

        @pl.when((u % 2 == 1) & (u >= 5) & ((u - 1) // 2 < line))
        def _():
            from_sides((u - 1) // 2)

        @pl.when(u % 4 == 2)
        def _():
            arrived(at_step(i), 1, 1)

        if line > 1:

            @pl.when(u == 2)
            def _():
                from_sides(zero + 1)

    def locate(u):
        z = at_step(u // 4)
        n = 4 * z + 2 * ((chip + u // 2) % 2) + core
        return z, n, n // 2, 1 - u % 2

    def analyze(u, slot, first=False):
        z, n, at, g = locate(u)
        before = jnp.maximum(n - 1, 0)
        from_info = jnp.where((g == 0) & (n > 0), 1.0, 0.0)
        from_blk = jnp.where(g == 0, 0.0, 1.0)
        even, odd = [], []
        for c in range(2):
            base = c * rows
            tail = buf[at, 0, base + rows - 2 : base + rows, :]
            if not first:
                tail = tail * from_blk + infos[before, 2 * c : 2 * c + 2, :] * from_info
            r0 = buf[at, g, base : base + rows, :]
            r1 = jnp.concatenate([tail[1:2], buf[at, g, base : base + rows - 1, :]], axis=0)
            r2 = jnp.concatenate([tail, buf[at, g, base : base + rows - 2, :]], axis=0)
            even += [
                pltpu.roll(jnp.where(low, r1, r2), HOP, 1),
                pltpu.roll(jnp.where(low, r0, r1), HOP, 1),
            ]
            odd += [r1, r0]
        f_hi, f_lo = [], []
        for part in (even, odd):
            hi, lo = split(jnp.concatenate(part, axis=1))
            f_hi.append(hi)
            f_lo.append(lo)
        f_hi = jnp.concatenate(f_hi, axis=0)
        f_lo = jnp.concatenate(f_lo, axis=0)
        dot = functools.partial(jnp.dot, preferred_element_type=jnp.float32)
        upper = dot3(f_hi, f_lo, ty[0], ty[1], ((1,), (0,)))
        twice = dot(f_hi, txs[...])
        lower = twice[:, :LANES] + dot(f_lo, txs[:, :LANES]) + twice[:, LANES:]

        spec_y[slot] = upper
        spec_x[slot] = lower

    def build(u, slot, first=False):
        z, n, at, g = locate(u)
        if first:
            rel = infos[slab, 4:8, :] * jnp.where(core > 0, 1.0, 0.0)
            rel = jnp.concatenate([rel, rel], axis=0)
        else:
            rel = ends[z]
            for k in range(1, 4):
                drop = infos[4 * z + k, 4:8, :] * jnp.where(4 * z + k > n, 1.0, 0.0)
                rel = rel - jnp.concatenate([drop, drop], axis=0)
        stamp = rel.astype(jnp.int32)
        t = (spread(stamp, 2) + HOP * jlane) & (period - 1)
        phq = rotation((turn * t) & (2 * period - 1), 2 * period)
        phx = [rotation(kchan * ((stamp + HOP * (jsub + p)) & (NCH - 1)), NCH) for p in range(2)]
        phy = [rotation(lchan * ((stamp + HOP * (jsub + p)) & (NCH - 1)), NCH) for p in range(2)]

        zrs, zis, kxs = [], [], []
        for p in range(2):
            c, s = (spread(v, rows // 8) for v in phy[p])
            part = spec_y[slot, p * rows : (p + 1) * rows, :]
            yr, yi = part[:, :LW], part[:, LW:]
            zrs.append(yr * c - yi * s)
            zis.append(yr * s + yi * c)
            c, s = spread(phx[p][0], rows // 8), spread(phx[p][1] * ksign, rows // 8)
            part = spec_x[slot, p * rows : (p + 1) * rows, :]
            kxs.append(part * c + pltpu.roll(part, own_w, 1) * s)
        zr_hi, zr_lo = split(jnp.concatenate(zrs, axis=0))
        zi_hi, zi_lo = split(jnp.concatenate(zis, axis=0))

        def weights(zr, zi):
            return jnp.concatenate(
                [jnp.concatenate([zr, -zi], 1), jnp.concatenate([zi, zr], 1)], axis=0
            )

        w_hi[slot] = weights(zr_hi, zi_hi)
        w_lo[slot] = weights(zr_lo, zi_lo)
        x = jnp.concatenate(kxs, axis=0).T
        xr, xi = x[:own_w], x[own_w:]
        c, s = phq[0][8:9], phq[1][8:9]
        ur = xr * c - xi * s
        ui = xr * s + xi * c

        def put(q, real, imag):
            hi, lo = split(jnp.concatenate([real, imag], axis=1))
            a_hi[slot, q * own_w : (q + 1) * own_w, :] = hi
            a_lo[slot, q * own_w : (q + 1) * own_w, :] = lo

        def turned(c):
            for m in range(c * cut // 2, (c + 1) * cut // 2):
                c, s = phq[0][m : m + 1], phq[1][m : m + 1]
                rc, rs, ic, is_ = ur * c, ur * s, ui * c, ui * s
                put(pairs + m, rc - is_, ic + rs)
                put(pairs - 1 - m, rc + is_, ic - rs)

        return turned

    def accumulate(slot, c):
        count = cut * own_w
        at = pl.ds(c * count if isinstance(c, int) else pl.multiple_of(c * count, count), count)
        part = dot3(a_hi[slot, at, :], a_lo[slot, at, :], w_hi[slot], w_lo[slot], ((1,), (0,)))
        sr = part[:, :LW].reshape(cut, own_w, LW)
        si = part[:, LW:].reshape(cut, own_w, LW)
        half, piece = c // cuts, c % cuts
        q = pl.ds(piece * cut, cut)
        acc[half, 0, q] = jnp.maximum(acc[half, 0, q], sr * sr + si * si)
        acc[half, 1, q] = acc[half, 1, q] + sr
        acc[half, 2, q] = acc[half, 2, q] + si

    units = 4 * line

    def step(u, carry):
        slot = u % 2
        events(u + 2)
        accumulate(slot, 0)
        turned = build(u + 1, 1 - slot)
        analyze(u + 2, slot)
        turned(0)
        for c in range(1, 2 * cuts):
            accumulate(slot, c)
            turned(c)
        return carry

    @pl.when(grp != last)
    def _():
        to_group.wait_recv()
        to_partner.start()

    info_copy(slab + 1 - 2 * core, 1, 0, 1, partner).wait_recv()
    others(lambda p, i: to_chip(p, i).start())
    for copy in tables:
        copy.wait()
    if line > 1:
        from_line(zero + 1)
    from_sides(zero)
    analyze(zero, 0, True)
    reach(zero)
    if line > 2:
        from_line(zero + 2)
    turned = build(zero, 0, True)
    analyze(zero + 1, 1)
    for c in range(2 * cuts):
        turned(c)
    lax.fori_loop(0, units - 2, step, 0)
    turned = build(zero + units - 1, 1)
    for c in range(2 * cuts):
        turned(c)
    def swap(c):
        q = pl.ds(c * cut, cut)
        return [
            remote(
                acc.at[1 - core, k, q], got.at[k, q], swap_sem.at[0, 3 * c + k], swap_sem.at[1, 3 * c + k], partner
            )
            for k in range(3)
        ]

    for c in range(cuts):
        for slot in range(2):
            accumulate(slot, (1 - core) * cuts + c)
        for copy in swap(c):
            copy.start()
    for c in range(cuts):
        for slot in range(2):
            accumulate(slot, core * cuts + c)

    total = jnp.zeros((4, LANES), jnp.float32)
    for k in range(4):
        total = total + infos[k, 4:8, :]
    stamp = (jnp.concatenate([total, total], axis=0) - ends[0]).astype(jnp.int32) & (period - 1)
    klane = lax.broadcasted_iota(jnp.int32, (own_w, LANES), 1)
    ksub = grp * own_w + lax.broadcasted_iota(jnp.int32, (own_w, LANES), 0)
    kl = rotation((ksub - KW - klane) * spread(stamp, own_w // 8), NCH)
    qrow = slab * own_bins + lax.broadcasted_iota(jnp.int32, (8, LANES), 0)
    ql = rotation(qrow * stamp, period)
    scale = 1.0 / math.sqrt(slabs * BLOCKS)
    for c in range(cuts):
        for copy in swap(c):
            copy.wait_recv()
    held[...] = jnp.sqrt(jnp.maximum(acc[core, 0], got[0]))
    for q in range(own_bins):
        c, s = ql[0][q : q + 1] * scale, ql[1][q : q + 1] * scale
        fc = kl[0] * c - kl[1] * s
        fs = kl[0] * s + kl[1] * c
        real = acc[core, 1, q] + got[1, q]
        imag = acc[core, 2, q] + got[2, q]
        coh[0, q] = real * fc - imag * fs
        coh[1, q] = real * fs + imag * fc

    @pl.when(grp == last)
    def _():
        to_group.wait_send()

    to_partner.wait_send()
    others(lambda p, i: to_chip(p, i).wait_send())
    run(1, line, lambda i: line_copy(i).wait_send())

    def sent(i):
        to_x(i).wait_send()
        to_y(i).wait_send()
        diagonal_x(i).wait_send()

    run(0, line, sent)
    for c in range(cuts):
        for copy in swap(c):
            copy.wait_send()


def on_device(capture, dropped):
    slabs = lax.axis_size("slab")
    groups = lax.axis_size("grp")
    own_bins = Q // slabs
    own_w = KW // groups
    local = capture.shape[1] // LANES
    to_real, to_imag = dft_tables()
    ty = np.concatenate([to_real[:, KW:], to_imag[:, KW:]], 1)
    tx = np.stack(
        [
            np.concatenate(
                [to_real[:, g * own_w : (g + 1) * own_w], to_imag[:, g * own_w : (g + 1) * own_w]], 1
            )
            for g in range(groups)
        ]
    ) / math.sqrt(Q)
    ty = jnp.stack(split_np(ty))
    txs = jnp.concatenate(split_np(tx), axis=2)
    blocks = capture.reshape(2, local, LANES).transpose(1, 0, 2)
    dma = pltpu.SemaphoreType.DMA
    line = slabs // 4
    count = 2 * own_bins * own_w
    slot = [pltpu.VMEM((2, count, 2 * Q), jnp.bfloat16)] * 2
    slot = slot + [pltpu.VMEM((2, 2 * Q, 2 * LW), jnp.bfloat16)] * 2
    slot = slot + [pltpu.VMEM((2, Q, w), jnp.float32) for w in (2 * LW, LANES)]
    held, coherent = pl.pallas_call(
        functools.partial(surfaces, slabs=slabs, groups=groups, own_bins=own_bins, own_w=own_w),
        out_shape=[
            jax.ShapeDtypeStruct((own_bins, own_w, LW), jnp.float32),
            jax.ShapeDtypeStruct((2, own_bins, own_w, LW), jnp.float32),
        ],
        in_specs=[pl.BlockSpec(memory_space=space) for space in (pltpu.HBM, pltpu.SMEM, pltpu.HBM, pltpu.HBM)],
        out_specs=[pl.BlockSpec(memory_space=pltpu.VMEM)] * 2,
        scratch_shapes=[
            pltpu.VMEM((local, 2, LANES), jnp.float32),
            pltpu.VMEM((slabs // 2, groups, 2 * local, LANES), jnp.float32),
            pltpu.VMEM((slabs, 8, LANES), jnp.float32),
            pltpu.VMEM((2, 3, own_bins, own_w, LW), jnp.float32),
            pltpu.VMEM((3, own_bins, own_w, LW), jnp.float32),
            pltpu.VMEM((line, 8, LANES), jnp.float32),
            pltpu.VMEM(ty.shape, jnp.bfloat16),
            pltpu.VMEM(txs.shape[1:], jnp.bfloat16),
            *slot,
            dma((line,)),
            dma((line,)),
            dma((line,)),
            dma((line,)),
            dma((slabs // 2, groups)),
            dma((slabs // 2 + 1,)),
            dma((slabs // 2 + 2,)),
            dma((2, 3 * own_bins)),
            dma((3,)),
        ],
        compiler_params=pltpu.CompilerParams(
            collective_id=0, has_side_effects=True, vmem_limit_bytes=VMEM_LIMIT
        ),
    )(
        blocks,
        dropped,
        ty,
        txs,
    )
    return held, coherent


def solution(mesh):
    in_specs = (P(None, ("slab", "grp")), P("slab"))
    out_specs = (P("slab", "grp", None), P(None, "slab", "grp", None))
    return jax.shard_map(
        on_device, mesh=mesh, in_specs=in_specs, out_specs=out_specs, check_vma=False
    )
```

```python
import functools
import math

import jax
import jax.numpy as jnp
import numpy as np
from jax import lax
from jax.experimental import pallas as pl
from jax.experimental.pallas import tpu as pltpu
from jax.sharding import PartitionSpec as P

NCH = 256
HOP = 64
KW = 128
LW = 128
Q = 128
BLOCKS = 2
LANES = 128
VMEM_LIMIT = 67043328 - 11300 * 2**10


def split_np(table):
    hi = table.astype(jnp.bfloat16)
    lo = (table - hi.astype(np.float64)).astype(jnp.bfloat16)
    return jnp.asarray(hi), jnp.asarray(lo)


def split(values):
    hi = values.astype(jnp.bfloat16)
    lo = (values - hi.astype(jnp.float32)).astype(jnp.bfloat16)
    return hi, lo


def dft_tables():
    i = np.arange(NCH)
    w = 0.5 - 0.5 * np.cos(2.0 * np.pi * i / NCH)
    w = w / np.sqrt(np.sum(w * w))
    turns = (i[:, None] * i[None, :] % NCH) * (2.0 * np.pi / NCH)
    cos, sin = w[:, None] * np.cos(turns), w[:, None] * np.sin(turns)
    to_real = np.concatenate([cos, sin], 0)
    to_imag = np.concatenate([-sin, cos], 0)
    return to_real, to_imag


def dot3(a_hi, a_lo, b_hi, b_lo, dims):
    dot = functools.partial(
        lax.dot_general, dimension_numbers=(dims, ((), ())), preferred_element_type=jnp.float32
    )
    return dot(a_hi, b_hi) + dot(a_lo, b_hi) + dot(a_hi, b_lo)


def cos_turns(turns, period):
    v = (jnp.abs(turns.astype(jnp.float32) * (1.0 / period) - 0.5) - 0.25) * (2.0 * math.pi)
    v2 = v * v
    total = jnp.full_like(v, 1.0 / math.factorial(13))
    for order in (11, 9, 7, 5, 3, 1):
        sign = 1.0 if order % 4 == 1 else -1.0
        total = total * v2 + sign / math.factorial(order)
    return total * v


def rotation(turns, period):
    return cos_turns(turns & (period - 1), period), cos_turns((turns + period // 4) & (period - 1), period)

def surfaces(
    own_hbm, own_drop, ty_hbm, tx_hbm, held, coh,
    raw, buf, infos, acc, got, ends, ty, txs, *rest,
    slabs, groups, own_bins, own_w
):
    a_hi, a_lo, w_hi, w_lo, spec_y, spec_x = rest[:6]
    line_sem, x_sem, y_sem, diag_sem, recv_sem, isend_sem, irecv_sem, swap_sem, load_sem = rest[6:]
    slab, grp = lax.axis_index("slab"), lax.axis_index("grp")
    bits = slabs.bit_length() - 1
    line = slabs // 4
    rows = Q // 2
    bins = 2 * own_bins
    pairs = bins // 2
    cut = min(4, own_bins)
    cuts = own_bins // cut
    period = Q * HOP
    last = groups - 1
    zero = slab * 0
    core = slab % 2
    chip = (slab // 2) % 2
    level = slab // 4
    partner = (slab + 1 - 2 * core, grp)
    beside = (slab + 2 - 4 * chip, grp)
    across = (slab, 1 - grp)

    place = slab // 2

    def load(src, dst, i):
        return pltpu.make_async_copy(src, dst, load_sem.at[i])

    own_load = load(own_hbm, raw, 2)
    own_load.start()
    tables = [load(ty_hbm, ty, 0), load(tx_hbm.at[grp], txs, 1)]
    for copy in tables:
        copy.start()

    def chip_at(p):
        return (2 * p + core, grp)

    barrier = pltpu.get_barrier_semaphore()

    def greet(target):
        pl.semaphore_signal(barrier, inc=1, device_id=target, device_id_type=pl.DeviceIdType.MESH)

    def others(act):
        def body(i, carry):
            act((place + i) % (slabs // 2), i)
            return carry

        lax.fori_loop(1, slabs // 2, body, 0)

    greet(partner)
    greet(across)
    others(lambda p, i: greet(chip_at(p)))

    def at_step(i):
        return jnp.where(i <= level, level - i, i)

    def remote(src, dst, send, recv, target):
        return pltpu.make_async_remote_copy(
            src_ref=src, dst_ref=dst, send_sem=send, recv_sem=recv,
            device_id=target, device_id_type=pl.DeviceIdType.MESH,
        )

    def moved(z, dx, dg, send, target):
        at = 2 * z + (chip + dx) % 2
        g = (grp + dg) % groups
        return remote(buf.at[at, g], buf.at[at, g], send, recv_sem.at[at, g], target)

    def arrived(z, dx, dg):
        moved(z, dx, dg, line_sem.at[0], partner).wait_recv()

    def info_copy(first, count, send, recv, target):
        piece = infos.at[pl.ds(first, count)]
        return remote(piece, piece, isend_sem.at[send], irecv_sem.at[recv], target)

    chips = slabs // 2
    to_group = info_copy(slab, 1, 0, 0, across)
    to_partner = info_copy(slab, 1, chips, 1, partner)

    def to_chip(p, i):
        return info_copy(2 * place, 2, i, 2 + place, chip_at(p))

    def info_arrived(p):
        info_copy(2 * p, 2, 0, 2 + p, partner).wait_recv()

    def line_copy(i):
        return moved(level, 0, 0, line_sem.at[i], (slab + 4 * (at_step(i) - level), grp))

    def to_x(i):
        return moved(at_step(i), 0, 0, x_sem.at[i], beside)

    def to_y(i):
        return moved(at_step(i), 0, 0, y_sem.at[i], across)

    def diagonal(i):
        odd = at_step(i) % 2
        return moved(at_step(i), odd, 1 - odd, diag_sem.at[i], (slab + (2 - 4 * chip) * (1 - odd), grp + odd * (1 - 2 * grp)))

    def from_line(i):
        arrived(at_step(i), 0, 0)
        to_x(i).start()
        to_y(i).start()

    def from_sides(i):
        odd = at_step(i) % 2
        arrived(at_step(i), odd, 1 - odd)
        diagonal(i).start()
        arrived(at_step(i), 1 - odd, odd)

    def run(first, end, act):
        def body(i, carry):
            act(i)
            return carry

        lax.fori_loop(first, end, body, 0)

    def reach(i):
        z = at_step(i)
        down = i <= level
        first = 2 * z - jnp.where(down & (z > 0), 1, 0)
        end = 2 * z + jnp.where(down & (i > 0), 1, 2)

        def wait(p):
            @pl.when(p != place)
            def _():
                info_arrived(p)

        run(first, end, wait)
        before = jnp.where(down, z + 1, z - 1)
        summed = jnp.where(down, z + 1, z)
        total = jnp.zeros((4, LANES), jnp.float32)
        for k in range(4):
            total = total + infos[4 * jnp.where(i == 0, z, summed) + k, 4:8, :] * jnp.where(
                (i > 0) | (4 * z + k > slab - core), 1.0, 0.0
            )
        base = ends[jnp.where(i == 0, z, before)] * jnp.where(i == 0, 0.0, 1.0)
        ends[z] = base + jnp.concatenate([total, total], axis=0) * jnp.where(down & (i > 0), -1.0, 1.0)

    ends[...] = jnp.zeros_like(ends)
    acc[...] = jnp.zeros_like(acc)
    own_load.wait()
    for c in range(2):
        buf[place, grp, c * rows : (c + 1) * rows, :] = raw[:, c, :]

    @pl.when(grp == last)
    def _():
        infos[slab] = jnp.concatenate(
            [
                raw[rows - 2 :, 0, :],
                raw[rows - 2 :, 1, :],
                jnp.broadcast_to(own_drop[0].astype(jnp.float32), (4, LANES)),
            ],
            axis=0,
        )

    pl.semaphore_wait(barrier, chips + 1)

    @pl.when(grp == last)
    def _():
        to_group.start()
        to_partner.start()

    to_x(0).start()
    to_y(0).start()
    run(1, line, lambda i: line_copy(i).start())

    lane = lax.broadcasted_iota(jnp.int32, (rows, LANES), 1)
    low = lane < HOP
    jlane = lax.broadcasted_iota(jnp.int32, (16, Q), 1)
    jlane = 2 * (jlane & (rows - 1)) + (jlane >= rows).astype(jnp.int32)
    turn = lax.broadcasted_iota(jnp.int32, (16, Q), 0)
    turn = jnp.where(turn < 8, 2 * turn + 1, 2 * bins * (slab // 2) + bins - 1)
    lanes8 = lax.broadcasted_iota(jnp.int32, (8, LANES), 1)
    lchan = KW + lanes8
    kchan = grp * own_w + (lanes8 & (own_w - 1))
    ksign = jnp.where(lanes8 < own_w, -1.0, 1.0)
    jsub = 2 * lax.broadcasted_iota(jnp.int32, (8, LANES), 0)

    def spread(array, count):
        return jnp.concatenate([array] * count, axis=0)

    def events(i, w):
        if w == 0:
            arrived(at_step(i), 1, 1)

            @pl.when((i == 0) & (line > 1))
            def _():
                from_sides(i + 1)

        elif w == 2:

            @pl.when(i + 1 < line)
            def _():
                reach(i + 1)

        else:
            j = 2 * i + (w + 1) // 2

            @pl.when(j + 2 < line)
            def _():
                from_line(j + 2)

            @pl.when((j > 1) & (j < line))
            def _():
                from_sides(j)

    def locate(u):
        z = at_step(u // 4)
        n = 4 * z + 2 * ((chip + u // 2) % 2) + core
        return z, n, n // 2, 1 - u % 2

    def analyze(u, slot, first=False):
        z, n, at, g = locate(u)
        before = jnp.maximum(n - 1, 0)
        from_info = jnp.where((g == 0) & (n > 0), 1.0, 0.0)
        from_blk = jnp.where(g == 0, 0.0, 1.0)
        even, odd = [], []
        for c in range(2):
            base = c * rows
            tail = buf[at, 0, base + rows - 2 : base + rows, :]
            if not first:
                tail = tail * from_blk + infos[before, 2 * c : 2 * c + 2, :] * from_info
            r0 = buf[at, g, base : base + rows, :]
            r1 = jnp.concatenate([tail[1:2], buf[at, g, base : base + rows - 1, :]], axis=0)
            r2 = jnp.concatenate([tail, buf[at, g, base : base + rows - 2, :]], axis=0)
            even += [
                pltpu.roll(jnp.where(low, r1, r2), HOP, 1),
                pltpu.roll(jnp.where(low, r0, r1), HOP, 1),
            ]
            odd += [r1, r0]
        f_hi, f_lo = [], []
        for part in (even, odd):
            hi, lo = split(jnp.concatenate(part, axis=1))
            f_hi.append(hi)
            f_lo.append(lo)
        f_hi = jnp.concatenate(f_hi, axis=0)
        f_lo = jnp.concatenate(f_lo, axis=0)
        dot = functools.partial(jnp.dot, preferred_element_type=jnp.float32)
        upper = dot3(f_hi, f_lo, ty[0], ty[1], ((1,), (0,)))

        spec_y[slot] = upper

        def finish():
            twice = dot(f_hi, txs[...])
            spec_x[slot] = twice[:, :LANES] + dot(f_lo, txs[:, :LANES]) + twice[:, LANES:]

        return finish

    def build(u, slot, first=False):
        z, n, at, g = locate(u)
        if first:
            rel = infos[slab, 4:8, :] * jnp.where(core > 0, 1.0, 0.0)
            rel = jnp.concatenate([rel, rel], axis=0)
        else:
            rel = ends[z]
            for k in range(1, 4):
                drop = infos[4 * z + k, 4:8, :] * jnp.where(4 * z + k > n, 1.0, 0.0)
                rel = rel - jnp.concatenate([drop, drop], axis=0)
        stamp = rel.astype(jnp.int32)
        t = (spread(stamp, 2) + HOP * jlane) & (period - 1)
        phq = rotation((turn * t) & (2 * period - 1), 2 * period)
        phx = [rotation(kchan * ((stamp + HOP * (jsub + p)) & (NCH - 1)), NCH) for p in range(2)]
        phy = [rotation(lchan * ((stamp + HOP * (jsub + p)) & (NCH - 1)), NCH) for p in range(2)]

        zrs, zis, kxs = [], [], []
        for p in range(2):
            c, s = (spread(v, rows // 8) for v in phy[p])
            part = spec_y[slot, p * rows : (p + 1) * rows, :]
            yr, yi = part[:, :LW], part[:, LW:]
            zrs.append(yr * c - yi * s)
            zis.append(yr * s + yi * c)
            c, s = spread(phx[p][0], rows // 8), spread(phx[p][1] * ksign, rows // 8)
            part = spec_x[slot, p * rows : (p + 1) * rows, :]
            kxs.append(part * c + pltpu.roll(part, own_w, 1) * s)
        zr_hi, zr_lo = split(jnp.concatenate(zrs, axis=0))
        zi_hi, zi_lo = split(jnp.concatenate(zis, axis=0))

        def weights(zr, zi):
            return jnp.concatenate(
                [jnp.concatenate([zr, -zi], 1), jnp.concatenate([zi, zr], 1)], axis=0
            )

        w_hi[slot] = weights(zr_hi, zi_hi)
        w_lo[slot] = weights(zr_lo, zi_lo)
        x = jnp.concatenate(kxs, axis=0).T
        xr, xi = x[:own_w], x[own_w:]
        c, s = phq[0][8:9], phq[1][8:9]
        ur = xr * c - xi * s
        ui = xr * s + xi * c

        def put(q, real, imag):
            hi, lo = split(jnp.concatenate([real, imag], axis=1))
            a_hi[slot, q * own_w : (q + 1) * own_w, :] = hi
            a_lo[slot, q * own_w : (q + 1) * own_w, :] = lo

        def turned(c):
            for m in range(c * cut // 2, (c + 1) * cut // 2):
                c, s = phq[0][m : m + 1], phq[1][m : m + 1]
                rc, rs, ic, is_ = ur * c, ur * s, ui * c, ui * s
                put(pairs + m, rc - is_, ic + rs)
                put(pairs - 1 - m, rc + is_, ic - rs)

        return turned

    def accumulate(slot, c, late):
        count = cut * own_w
        at = pl.ds(c * count if isinstance(c, int) else pl.multiple_of(c * count, count), count)
        hi = a_hi[slot, at, :]
        dot = functools.partial(jnp.dot, preferred_element_type=jnp.float32)
        both = jnp.concatenate([hi, a_lo[slot, at, :]], axis=0)
        if late:
            once = dot(hi, w_lo[slot])
            twice = dot(both, w_hi[slot])
        else:
            twice = dot(both, w_hi[slot])
            once = dot(hi, w_lo[slot])
        part = twice[:count] + twice[count:] + once
        sr = part[:, :LW].reshape(cut, own_w, LW)
        si = part[:, LW:].reshape(cut, own_w, LW)
        half, piece = c // cuts, c % cuts
        q = pl.ds(piece * cut, cut)
        acc[half, 0, q] = jnp.maximum(acc[half, 0, q], sr * sr + si * si)
        acc[half, 1, q] = acc[half, 1, q] + sr
        acc[half, 2, q] = acc[half, 2, q] + si

    units = 4 * line

    def step(i, w, slot):
        u = 4 * i + w
        slot = u % 2
        events(i, w)
        accumulate(slot, 0, 0)
        turned = build(u + 1, 1 - slot)
        finish = analyze(u + 2, slot)
        turned(0)
        for c in range(1, 2 * cuts):
            accumulate(slot, c, c % 2)
            if c == 1:
                finish()
            turned(c)
        return 1 - slot

    def steps(i, slot):
        for w in range(4):
            slot = step(i, w, slot)
        return slot

    @pl.when(grp != last)
    def _():
        to_group.wait_recv()
        to_partner.start()

    info_copy(slab + 1 - 2 * core, 1, 0, 1, partner).wait_recv()
    others(lambda p, i: to_chip(p, i).start())
    for copy in tables:
        copy.wait()
    if line > 1:
        from_line(zero + 1)
    from_sides(zero)
    analyze(zero, 0, True)()
    reach(zero)
    if line > 2:
        from_line(zero + 2)
    turned = build(zero, 0, True)
    analyze(zero + 1, 1)()
    for c in range(2 * cuts):
        turned(c)
    slot = lax.fori_loop(0, line - 1, steps, zero)
    slot = step(zero + line - 1, 0, slot)
    step(zero + line - 1, 1, slot)
    slot = 0
    turned = build(zero + units - 1, 1 - slot)
    for c in range(2 * cuts):
        turned(c)
    def swap(c):
        q = pl.ds(c * cut, cut)
        return [
            remote(
                acc.at[1 - core, k, q], got.at[k, q], swap_sem.at[0, 3 * c + k], swap_sem.at[1, 3 * c + k], partner
            )
            for k in range(3)
        ]

    for c in range(cuts):
        for late, other in enumerate((slot, 1 - slot)):
            accumulate(other, (1 - core) * cuts + c, late)
        for copy in swap(c):
            copy.start()
    for c in range(cuts):
        for late, other in enumerate((slot, 1 - slot)):
            accumulate(other, core * cuts + c, late)

    total = jnp.zeros((4, LANES), jnp.float32)
    for k in range(4):
        total = total + infos[k, 4:8, :]
    stamp = (jnp.concatenate([total, total], axis=0) - ends[0]).astype(jnp.int32) & (period - 1)
    klane = lax.broadcasted_iota(jnp.int32, (own_w, LANES), 1)
    ksub = grp * own_w + lax.broadcasted_iota(jnp.int32, (own_w, LANES), 0)
    kl = rotation((ksub - KW - klane) * spread(stamp, own_w // 8), NCH)
    qrow = slab * own_bins + lax.broadcasted_iota(jnp.int32, (8, LANES), 0)
    ql = rotation(qrow * stamp, period)
    scale = 1.0 / math.sqrt(slabs * BLOCKS)
    for c in range(cuts):
        for copy in swap(c):
            copy.wait_recv()
    held[...] = jnp.sqrt(jnp.maximum(acc[core, 0], got[0]))
    for q in range(own_bins):
        c, s = ql[0][q : q + 1] * scale, ql[1][q : q + 1] * scale
        fc = kl[0] * c - kl[1] * s
        fs = kl[0] * s + kl[1] * c
        real = acc[core, 1, q] + got[1, q]
        imag = acc[core, 2, q] + got[2, q]
        coh[0, q] = real * fc - imag * fs
        coh[1, q] = real * fs + imag * fc

    @pl.when(grp == last)
    def _():
        to_group.wait_send()

    to_partner.wait_send()
    others(lambda p, i: to_chip(p, i).wait_send())
    run(1, line, lambda i: line_copy(i).wait_send())

    def sent(i):
        to_x(i).wait_send()
        to_y(i).wait_send()
        diagonal(i).wait_send()

    run(0, line, sent)
    for c in range(cuts):
        for copy in swap(c):
            copy.wait_send()


def put_out(held, coh, held_out, coh_out, sems):
    copies = [
        pltpu.make_async_copy(held, held_out, sems.at[0]),
        pltpu.make_async_copy(coh, coh_out, sems.at[1]),
    ]
    for copy in copies:
        copy.start()
    for copy in copies:
        copy.wait()


def on_device(capture, dropped):
    slabs = lax.axis_size("slab")
    groups = lax.axis_size("grp")
    own_bins = Q // slabs
    own_w = KW // groups
    local = capture.shape[1] // LANES
    to_real, to_imag = dft_tables()
    ty = np.concatenate([to_real[:, KW:], to_imag[:, KW:]], 1)
    tx = np.stack(
        [
            np.concatenate(
                [to_real[:, g * own_w : (g + 1) * own_w], to_imag[:, g * own_w : (g + 1) * own_w]], 1
            )
            for g in range(groups)
        ]
    ) / math.sqrt(Q)
    ty = jnp.stack(split_np(ty))
    txs = jnp.concatenate(split_np(tx), axis=2)
    blocks = capture.reshape(2, local, LANES).transpose(1, 0, 2)
    dma = pltpu.SemaphoreType.DMA
    line = slabs // 4
    count = 2 * own_bins * own_w
    slot = [pltpu.VMEM((2, count, 2 * Q), jnp.bfloat16)] * 2
    slot = slot + [pltpu.VMEM((2, 2 * Q, 2 * LW), jnp.bfloat16)] * 2
    slot = slot + [pltpu.VMEM((2, Q, w), jnp.float32) for w in (2 * LW, LANES)]
    results = pl.pallas_call(
        functools.partial(surfaces, slabs=slabs, groups=groups, own_bins=own_bins, own_w=own_w),
        out_shape=[
            jax.ShapeDtypeStruct((own_bins, own_w, LW), jnp.float32),
            jax.ShapeDtypeStruct((2, own_bins, own_w, LW), jnp.float32),
        ],
        in_specs=[pl.BlockSpec(memory_space=space) for space in (pltpu.HBM, pltpu.SMEM, pltpu.HBM, pltpu.HBM)],
        out_specs=[pl.BlockSpec(memory_space=pltpu.VMEM)] * 2,
        scratch_shapes=[
            pltpu.VMEM((local, 2, LANES), jnp.float32),
            pltpu.VMEM((slabs // 2, groups, 2 * local, LANES), jnp.float32),
            pltpu.VMEM((slabs, 8, LANES), jnp.float32),
            pltpu.VMEM((2, 3, own_bins, own_w, LW), jnp.float32),
            pltpu.VMEM((3, own_bins, own_w, LW), jnp.float32),
            pltpu.VMEM((line, 8, LANES), jnp.float32),
            pltpu.VMEM(ty.shape, jnp.bfloat16),
            pltpu.VMEM(txs.shape[1:], jnp.bfloat16),
            *slot,
            dma((line,)),
            dma((line,)),
            dma((line,)),
            dma((line,)),
            dma((slabs // 2, groups)),
            dma((slabs // 2 + 1,)),
            dma((slabs // 2 + 2,)),
            dma((2, 3 * own_bins)),
            dma((3,)),
        ],
        compiler_params=pltpu.CompilerParams(
            collective_id=0, has_side_effects=True, vmem_limit_bytes=VMEM_LIMIT
        ),
    )(
        blocks,
        dropped,
        ty,
        txs,
    )
    return pl.pallas_call(
        put_out,
        out_shape=[jax.ShapeDtypeStruct(r.shape, r.dtype) for r in results],
        in_specs=[pl.BlockSpec(memory_space=pltpu.VMEM)] * 2,
        out_specs=[pl.BlockSpec(memory_space=pltpu.HBM)] * 2,
        scratch_shapes=[dma((2,))],
        compiler_params=pltpu.CompilerParams(vmem_limit_bytes=2**20),
    )(*results)


def solution(mesh):
    in_specs = (P(None, ("slab", "grp")), P("slab"))
    out_specs = (P("slab", "grp", None), P(None, "slab", "grp", None))
    return jax.shard_map(
        on_device, mesh=mesh, in_specs=in_specs, out_specs=out_specs, check_vma=False
    )
```

```python
import functools
import math

import jax
import jax.numpy as jnp
import numpy as np
from jax import lax
from jax.experimental import pallas as pl
from jax.experimental.pallas import tpu as pltpu
from jax.sharding import PartitionSpec as P

NCH = 256
HOP = 64
KW = 128
LW = 128
Q = 128
BLOCKS = 2
LANES = 128
VMEM_LIMIT = 67043328 - 11300 * 2**10


def split_np(table):
    hi = table.astype(jnp.bfloat16)
    lo = (table - hi.astype(np.float64)).astype(jnp.bfloat16)
    return jnp.asarray(hi), jnp.asarray(lo)


def split(values):
    hi = values.astype(jnp.bfloat16)
    lo = (values - hi.astype(jnp.float32)).astype(jnp.bfloat16)
    return hi, lo


def dft_tables():
    i = np.arange(NCH)
    w = 0.5 - 0.5 * np.cos(2.0 * np.pi * i / NCH)
    w = w / np.sqrt(np.sum(w * w))
    turns = (i[:, None] * i[None, :] % NCH) * (2.0 * np.pi / NCH)
    cos, sin = w[:, None] * np.cos(turns), w[:, None] * np.sin(turns)
    to_real = np.concatenate([cos, sin], 0)
    to_imag = np.concatenate([-sin, cos], 0)
    return to_real, to_imag


def dot3(a_hi, a_lo, b_hi, b_lo, dims):
    dot = functools.partial(
        lax.dot_general, dimension_numbers=(dims, ((), ())), preferred_element_type=jnp.float32
    )
    return dot(a_hi, b_hi) + dot(a_lo, b_hi) + dot(a_hi, b_lo)


def cos_turns(turns, period):
    v = (jnp.abs(turns.astype(jnp.float32) * (1.0 / period) - 0.5) - 0.25) * (2.0 * math.pi)
    v2 = v * v
    total = jnp.full_like(v, 1.0 / math.factorial(13))
    for order in (11, 9, 7, 5, 3, 1):
        sign = 1.0 if order % 4 == 1 else -1.0
        total = total * v2 + sign / math.factorial(order)
    return total * v


def rotation(turns, period):
    return cos_turns(turns & (period - 1), period), cos_turns((turns + period // 4) & (period - 1), period)

def surfaces(
    raw, own_drop, ty_hbm, tx_hbm, held, coh,
    buf, infos, acc, got, ends, ty, txs, *rest,
    slabs, groups, own_bins, own_w
):
    a_hi, a_lo, w_hi, w_lo, spec_y, spec_x = rest[:6]
    line_sem, x_sem, y_sem, diag_sem, recv_sem, isend_sem, irecv_sem, swap_sem, load_sem = rest[6:]
    slab, grp = lax.axis_index("slab"), lax.axis_index("grp")
    bits = slabs.bit_length() - 1
    line = slabs // 4
    rows = Q // 2
    bins = 2 * own_bins
    pairs = bins // 2
    cut = min(4, own_bins)
    cuts = own_bins // cut
    period = Q * HOP
    last = groups - 1
    zero = slab * 0
    core = slab % 2
    chip = (slab // 2) % 2
    level = slab // 4
    partner = (slab + 1 - 2 * core, grp)
    beside = (slab + 2 - 4 * chip, grp)
    across = (slab, 1 - grp)

    place = slab // 2

    def load(src, dst, i):
        return pltpu.make_async_copy(src, dst, load_sem.at[i])

    tables = [load(ty_hbm, ty, 0), load(tx_hbm.at[grp], txs, 1)]
    for copy in tables:
        copy.start()

    def chip_at(p):
        return (2 * p + core, grp)

    barrier = pltpu.get_barrier_semaphore()

    def greet(target):
        pl.semaphore_signal(barrier, inc=1, device_id=target, device_id_type=pl.DeviceIdType.MESH)

    def others(act):
        def body(i, carry):
            act((place + i) % (slabs // 2), i)
            return carry

        lax.fori_loop(1, slabs // 2, body, 0)

    greet(partner)
    greet(across)
    others(lambda p, i: greet(chip_at(p)))

    def at_step(i):
        return jnp.where(i <= level, level - i, i)

    def remote(src, dst, send, recv, target):
        return pltpu.make_async_remote_copy(
            src_ref=src, dst_ref=dst, send_sem=send, recv_sem=recv,
            device_id=target, device_id_type=pl.DeviceIdType.MESH,
        )

    def moved(z, dx, dg, send, target):
        at = 2 * z + (chip + dx) % 2
        g = (grp + dg) % groups
        return remote(buf.at[at, g], buf.at[at, g], send, recv_sem.at[at, g], target)

    def arrived(z, dx, dg):
        moved(z, dx, dg, line_sem.at[0], partner).wait_recv()

    def info_copy(first, count, send, recv, target):
        piece = infos.at[pl.ds(first, count)]
        return remote(piece, piece, isend_sem.at[send], irecv_sem.at[recv], target)

    chips = slabs // 2
    to_group = info_copy(slab, 1, 0, 0, across)
    to_partner = info_copy(slab, 1, chips, 1, partner)

    def to_chip(p, i):
        return info_copy(2 * place, 2, i, 2 + place, chip_at(p))

    def info_arrived(p):
        info_copy(2 * p, 2, 0, 2 + p, partner).wait_recv()

    def line_copy(i):
        return moved(level, 0, 0, line_sem.at[i], (slab + 4 * (at_step(i) - level), grp))

    def to_x(i):
        return moved(at_step(i), 0, 0, x_sem.at[i], beside)

    def to_y(i):
        return moved(at_step(i), 0, 0, y_sem.at[i], across)

    def diagonal(i):
        odd = at_step(i) % 2
        return moved(at_step(i), odd, 1 - odd, diag_sem.at[i], (slab + (2 - 4 * chip) * (1 - odd), grp + odd * (1 - 2 * grp)))

    def from_line(i):
        arrived(at_step(i), 0, 0)
        to_x(i).start()
        to_y(i).start()

    def from_sides(i):
        odd = at_step(i) % 2
        arrived(at_step(i), odd, 1 - odd)
        diagonal(i).start()
        arrived(at_step(i), 1 - odd, odd)

    def run(first, end, act):
        def body(i, carry):
            act(i)
            return carry

        lax.fori_loop(first, end, body, 0)

    def reach(i):
        z = at_step(i)
        down = i <= level
        first = 2 * z - jnp.where(down & (z > 0), 1, 0)
        end = 2 * z + jnp.where(down & (i > 0), 1, 2)

        def wait(p):
            @pl.when(p != place)
            def _():
                info_arrived(p)

        run(first, end, wait)
        before = jnp.where(down, z + 1, z - 1)
        summed = jnp.where(down, z + 1, z)
        total = jnp.zeros((4, LANES), jnp.float32)
        for k in range(4):
            total = total + infos[4 * jnp.where(i == 0, z, summed) + k, 4:8, :] * jnp.where(
                (i > 0) | (4 * z + k > slab - core), 1.0, 0.0
            )
        base = ends[jnp.where(i == 0, z, before)] * jnp.where(i == 0, 0.0, 1.0)
        ends[z] = base + jnp.concatenate([total, total], axis=0) * jnp.where(down & (i > 0), -1.0, 1.0)

    for c in range(2):
        buf[place, grp, c * rows : (c + 1) * rows, :] = raw[:, c, :]

    @pl.when(grp == last)
    def _():
        infos[slab] = jnp.concatenate(
            [
                raw[rows - 2 :, 0, :],
                raw[rows - 2 :, 1, :],
                jnp.broadcast_to(own_drop[0].astype(jnp.float32), (4, LANES)),
            ],
            axis=0,
        )

    pl.semaphore_wait(barrier, chips + 1)

    @pl.when(grp == last)
    def _():
        to_group.start()
        to_partner.start()

    to_x(0).start()
    to_y(0).start()
    run(1, line, lambda i: line_copy(i).start())
    ends[...] = jnp.zeros_like(ends)
    acc[...] = jnp.zeros_like(acc)

    lane = lax.broadcasted_iota(jnp.int32, (rows, LANES), 1)
    low = lane < HOP
    jlane = lax.broadcasted_iota(jnp.int32, (16, Q), 1)
    jlane = 2 * (jlane & (rows - 1)) + (jlane >= rows).astype(jnp.int32)
    turn = lax.broadcasted_iota(jnp.int32, (16, Q), 0)
    turn = jnp.where(turn < 8, 2 * turn + 1, 2 * bins * (slab // 2) + bins - 1)
    lanes8 = lax.broadcasted_iota(jnp.int32, (8, LANES), 1)
    lchan = KW + lanes8
    kchan = grp * own_w + (lanes8 & (own_w - 1))
    ksign = jnp.where(lanes8 < own_w, -1.0, 1.0)
    jsub = 2 * lax.broadcasted_iota(jnp.int32, (8, LANES), 0)

    def spread(array, count):
        return jnp.concatenate([array] * count, axis=0)

    def events(i, w, end=False):
        if end and w == 0:
            arrived(at_step(i), 1, 1)
        elif w == 0:
            from_sides(i + 1)
            reach(i + 1)
        elif w == 2:
            arrived(at_step(i), 1, 1)
        elif w == 3:

            @pl.when(i + 3 < line)
            def _():
                from_line(i + 3)

    def locate(u):
        h = u // 2
        far = ((h % 2 == 0) & (h > 0)) | (h == 2 * line - 1)
        i = jnp.where(far, (h - 1) // 2, (h + 1) // 2)
        z = at_step(i)
        n = 4 * z + 2 * ((chip + far.astype(jnp.int32)) % 2) + core
        return z, n, n // 2, 1 - u % 2

    def analyze(u, slot, first=False):
        z, n, at, g = locate(u)
        before = jnp.maximum(n - 1, 0)
        from_info = jnp.where((g == 0) & (n > 0), 1.0, 0.0)
        from_blk = jnp.where(g == 0, 0.0, 1.0)
        even, odd = [], []
        for c in range(2):
            base = c * rows
            tail = buf[at, 0, base + rows - 2 : base + rows, :]
            if not first:
                tail = tail * from_blk + infos[before, 2 * c : 2 * c + 2, :] * from_info
            r0 = buf[at, g, base : base + rows, :]
            r1 = jnp.concatenate([tail[1:2], buf[at, g, base : base + rows - 1, :]], axis=0)
            r2 = jnp.concatenate([tail, buf[at, g, base : base + rows - 2, :]], axis=0)
            even += [
                pltpu.roll(jnp.where(low, r1, r2), HOP, 1),
                pltpu.roll(jnp.where(low, r0, r1), HOP, 1),
            ]
            odd += [r1, r0]
        f_hi, f_lo = [], []
        for part in (even, odd):
            hi, lo = split(jnp.concatenate(part, axis=1))
            f_hi.append(hi)
            f_lo.append(lo)
        f_hi = jnp.concatenate(f_hi, axis=0)
        f_lo = jnp.concatenate(f_lo, axis=0)
        dot = functools.partial(jnp.dot, preferred_element_type=jnp.float32)
        upper = dot3(f_hi, f_lo, ty[0], ty[1], ((1,), (0,)))

        spec_y[slot] = upper

        def finish():
            twice = dot(f_hi, txs[...])
            spec_x[slot] = twice[:, :LANES] + dot(f_lo, txs[:, :LANES]) + twice[:, LANES:]

        return finish

    def build(u, slot, first=False):
        z, n, at, g = locate(u)
        if first:
            rel = infos[slab, 4:8, :] * jnp.where(core > 0, 1.0, 0.0)
            rel = jnp.concatenate([rel, rel], axis=0)
        else:
            rel = ends[z]
            for k in range(1, 4):
                drop = infos[4 * z + k, 4:8, :] * jnp.where(4 * z + k > n, 1.0, 0.0)
                rel = rel - jnp.concatenate([drop, drop], axis=0)
        stamp = rel.astype(jnp.int32)
        t = (spread(stamp, 2) + HOP * jlane) & (period - 1)
        phq = rotation((turn * t) & (2 * period - 1), 2 * period)
        phx = [rotation(kchan * ((stamp + HOP * (jsub + p)) & (NCH - 1)), NCH) for p in range(2)]
        phy = [rotation(lchan * ((stamp + HOP * (jsub + p)) & (NCH - 1)), NCH) for p in range(2)]

        zrs, zis, kxs = [], [], []
        for p in range(2):
            c, s = (spread(v, rows // 8) for v in phy[p])
            part = spec_y[slot, p * rows : (p + 1) * rows, :]
            yr, yi = part[:, :LW], part[:, LW:]
            zrs.append(yr * c - yi * s)
            zis.append(yr * s + yi * c)
            c, s = spread(phx[p][0], rows // 8), spread(phx[p][1] * ksign, rows // 8)
            part = spec_x[slot, p * rows : (p + 1) * rows, :]
            kxs.append(part * c + pltpu.roll(part, own_w, 1) * s)
        zr_hi, zr_lo = split(jnp.concatenate(zrs, axis=0))
        zi_hi, zi_lo = split(jnp.concatenate(zis, axis=0))

        def weights(zr, zi):
            return jnp.concatenate(
                [jnp.concatenate([zr, -zi], 1), jnp.concatenate([zi, zr], 1)], axis=0
            )

        w_hi[slot] = weights(zr_hi, zi_hi)
        w_lo[slot] = weights(zr_lo, zi_lo)
        x = jnp.concatenate(kxs, axis=0).T
        xr, xi = x[:own_w], x[own_w:]
        c, s = phq[0][8:9], phq[1][8:9]
        ur = xr * c - xi * s
        ui = xr * s + xi * c

        def put(q, real, imag):
            hi, lo = split(jnp.concatenate([real, imag], axis=1))
            a_hi[slot, q * own_w : (q + 1) * own_w, :] = hi
            a_lo[slot, q * own_w : (q + 1) * own_w, :] = lo

        def turned(c):
            for m in range(c * cut // 2, (c + 1) * cut // 2):
                c, s = phq[0][m : m + 1], phq[1][m : m + 1]
                rc, rs, ic, is_ = ur * c, ur * s, ui * c, ui * s
                put(pairs + m, rc - is_, ic + rs)
                put(pairs - 1 - m, rc + is_, ic - rs)

        return turned

    def accumulate(slot, c, late):
        count = cut * own_w
        at = pl.ds(c * count if isinstance(c, int) else pl.multiple_of(c * count, count), count)
        hi = a_hi[slot, at, :]
        dot = functools.partial(jnp.dot, preferred_element_type=jnp.float32)
        both = jnp.concatenate([hi, a_lo[slot, at, :]], axis=0)
        if late:
            once = dot(hi, w_lo[slot])
            twice = dot(both, w_hi[slot])
        else:
            twice = dot(both, w_hi[slot])
            once = dot(hi, w_lo[slot])
        part = twice[:count] + twice[count:] + once
        sr = part[:, :LW].reshape(cut, own_w, LW)
        si = part[:, LW:].reshape(cut, own_w, LW)
        half, piece = c // cuts, c % cuts
        q = pl.ds(piece * cut, cut)
        acc[half, 0, q] = jnp.maximum(acc[half, 0, q], sr * sr + si * si)
        acc[half, 1, q] = acc[half, 1, q] + sr
        acc[half, 2, q] = acc[half, 2, q] + si

    units = 4 * line

    def step(i, w, slot, end=False):
        u = 4 * i + w
        slot = u % 2
        events(i, w, end)
        accumulate(slot, 0, 0)
        turned = build(u + 1, 1 - slot)
        finish = analyze(u + 2, slot)
        turned(0)
        for c in range(1, 2 * cuts):
            accumulate(slot, c, c % 2)
            if c == 1:
                finish()
            turned(c)
        return 1 - slot

    def steps(i, slot):
        for w in range(4):
            slot = step(i, w, slot)
        return slot

    if line > 1:
        from_line(zero + 1)
    from_sides(zero)
    for copy in tables:
        copy.wait()
    analyze(zero, 0, True)()

    @pl.when(grp != last)
    def _():
        to_group.wait_recv()
        to_partner.start()

    info_copy(slab + 1 - 2 * core, 1, 0, 1, partner).wait_recv()
    others(lambda p, i: to_chip(p, i).start())
    if line > 2:
        from_line(zero + 2)
    reach(zero)
    turned = build(zero, 0, True)
    analyze(zero + 1, 1)()
    for c in range(2 * cuts):
        turned(c)
    slot = lax.fori_loop(0, line - 1, steps, zero)
    slot = step(zero + line - 1, 0, slot, True)
    step(zero + line - 1, 1, slot, True)
    slot = 0
    turned = build(zero + units - 1, 1 - slot)
    for c in range(2 * cuts):
        turned(c)
    def swap(c):
        q = pl.ds(c * cut, cut)
        return [
            remote(
                acc.at[1 - core, k, q], got.at[k, q], swap_sem.at[0, 3 * c + k], swap_sem.at[1, 3 * c + k], partner
            )
            for k in range(3)
        ]

    for c in range(cuts):
        for late, other in enumerate((slot, 1 - slot)):
            accumulate(other, (1 - core) * cuts + c, late)
        for copy in swap(c):
            copy.start()
    for c in range(cuts):
        for late, other in enumerate((slot, 1 - slot)):
            accumulate(other, core * cuts + c, late)

    total = jnp.zeros((4, LANES), jnp.float32)
    for k in range(4):
        total = total + infos[k, 4:8, :]
    stamp = (jnp.concatenate([total, total], axis=0) - ends[0]).astype(jnp.int32) & (period - 1)
    klane = lax.broadcasted_iota(jnp.int32, (own_w, LANES), 1)
    ksub = grp * own_w + lax.broadcasted_iota(jnp.int32, (own_w, LANES), 0)
    kl = rotation((ksub - KW - klane) * spread(stamp, own_w // 8), NCH)
    qrow = slab * own_bins + lax.broadcasted_iota(jnp.int32, (8, LANES), 0)
    ql = rotation(qrow * stamp, period)
    scale = 1.0 / math.sqrt(slabs * BLOCKS)
    for c in range(cuts):
        for copy in swap(c):
            copy.wait_recv()
    held[...] = jnp.sqrt(jnp.maximum(acc[core, 0], got[0]))
    for q in range(own_bins):
        c, s = ql[0][q : q + 1] * scale, ql[1][q : q + 1] * scale
        fc = kl[0] * c - kl[1] * s
        fs = kl[0] * s + kl[1] * c
        real = acc[core, 1, q] + got[1, q]
        imag = acc[core, 2, q] + got[2, q]
        coh[0, q] = real * fc - imag * fs
        coh[1, q] = real * fs + imag * fc

    @pl.when(grp == last)
    def _():
        to_group.wait_send()

    to_partner.wait_send()
    others(lambda p, i: to_chip(p, i).wait_send())
    run(1, line, lambda i: line_copy(i).wait_send())

    def sent(i):
        to_x(i).wait_send()
        to_y(i).wait_send()
        diagonal(i).wait_send()

    run(0, line, sent)
    for c in range(cuts):
        for copy in swap(c):
            copy.wait_send()


def put_out(held, coh, held_out, coh_out, sems):
    copies = [
        pltpu.make_async_copy(held, held_out, sems.at[0]),
        pltpu.make_async_copy(coh, coh_out, sems.at[1]),
    ]
    for copy in copies:
        copy.start()
    for copy in copies:
        copy.wait()


def on_device(capture, dropped):
    slabs = lax.axis_size("slab")
    groups = lax.axis_size("grp")
    own_bins = Q // slabs
    own_w = KW // groups
    local = capture.shape[1] // LANES
    to_real, to_imag = dft_tables()
    ty = np.concatenate([to_real[:, KW:], to_imag[:, KW:]], 1)
    tx = np.stack(
        [
            np.concatenate(
                [to_real[:, g * own_w : (g + 1) * own_w], to_imag[:, g * own_w : (g + 1) * own_w]], 1
            )
            for g in range(groups)
        ]
    ) / math.sqrt(Q)
    ty = jnp.stack(split_np(ty))
    txs = jnp.concatenate(split_np(tx), axis=2)
    blocks = capture.reshape(2, local, LANES).transpose(1, 0, 2)
    dma = pltpu.SemaphoreType.DMA
    line = slabs // 4
    count = 2 * own_bins * own_w
    slot = [pltpu.VMEM((2, count, 2 * Q), jnp.bfloat16)] * 2
    slot = slot + [pltpu.VMEM((2, 2 * Q, 2 * LW), jnp.bfloat16)] * 2
    slot = slot + [pltpu.VMEM((2, Q, w), jnp.float32) for w in (2 * LW, LANES)]
    results = pl.pallas_call(
        functools.partial(surfaces, slabs=slabs, groups=groups, own_bins=own_bins, own_w=own_w),
        out_shape=[
            jax.ShapeDtypeStruct((own_bins, own_w, LW), jnp.float32),
            jax.ShapeDtypeStruct((2, own_bins, own_w, LW), jnp.float32),
        ],
        in_specs=[pl.BlockSpec(memory_space=space) for space in (pltpu.VMEM, pltpu.SMEM, pltpu.HBM, pltpu.HBM)],
        out_specs=[pl.BlockSpec(memory_space=pltpu.VMEM)] * 2,
        scratch_shapes=[
            pltpu.VMEM((slabs // 2, groups, 2 * local, LANES), jnp.float32),
            pltpu.VMEM((slabs, 8, LANES), jnp.float32),
            pltpu.VMEM((2, 3, own_bins, own_w, LW), jnp.float32),
            pltpu.VMEM((3, own_bins, own_w, LW), jnp.float32),
            pltpu.VMEM((line, 8, LANES), jnp.float32),
            pltpu.VMEM(ty.shape, jnp.bfloat16),
            pltpu.VMEM(txs.shape[1:], jnp.bfloat16),
            *slot,
            dma((line,)),
            dma((line,)),
            dma((line,)),
            dma((line,)),
            dma((slabs // 2, groups)),
            dma((slabs // 2 + 1,)),
            dma((slabs // 2 + 2,)),
            dma((2, 3 * own_bins)),
            dma((2,)),
        ],
        compiler_params=pltpu.CompilerParams(
            collective_id=0, has_side_effects=True, vmem_limit_bytes=VMEM_LIMIT
        ),
    )(
        blocks,
        dropped,
        ty,
        txs,
    )
    return pl.pallas_call(
        put_out,
        out_shape=[jax.ShapeDtypeStruct(r.shape, r.dtype) for r in results],
        in_specs=[pl.BlockSpec(memory_space=pltpu.VMEM)] * 2,
        out_specs=[pl.BlockSpec(memory_space=pltpu.HBM)] * 2,
        scratch_shapes=[dma((2,))],
        compiler_params=pltpu.CompilerParams(vmem_limit_bytes=2**20),
    )(*results)


def solution(mesh):
    in_specs = (P(None, ("slab", "grp")), P("slab"))
    out_specs = (P("slab", "grp", None), P(None, "slab", "grp", None))
    return jax.shard_map(
        on_device, mesh=mesh, in_specs=in_specs, out_specs=out_specs, check_vma=False
    )
```

```python
import functools
import math

import jax
import jax.numpy as jnp
import numpy as np
from jax import lax
from jax.experimental import pallas as pl
from jax.experimental.pallas import tpu as pltpu
from jax.sharding import PartitionSpec as P

NCH = 256
HOP = 64
KW = 128
LW = 128
Q = 128
BLOCKS = 2
LANES = 128
VMEM_LIMIT = 67043328 - 11300 * 2**10


def split_np(table):
    hi = table.astype(jnp.bfloat16)
    lo = (table - hi.astype(np.float64)).astype(jnp.bfloat16)
    return jnp.asarray(hi), jnp.asarray(lo)


def split(values):
    hi = values.astype(jnp.bfloat16)
    lo = (values - hi.astype(jnp.float32)).astype(jnp.bfloat16)
    return hi, lo


def dft_tables():
    i = np.arange(NCH)
    w = 0.5 - 0.5 * np.cos(2.0 * np.pi * i / NCH)
    w = w / np.sqrt(np.sum(w * w))
    turns = (i[:, None] * i[None, :] % NCH) * (2.0 * np.pi / NCH)
    cos, sin = w[:, None] * np.cos(turns), w[:, None] * np.sin(turns)
    to_real = np.concatenate([cos, sin], 0)
    to_imag = np.concatenate([-sin, cos], 0)
    return to_real, to_imag


def dot3(a_hi, a_lo, b_hi, b_lo, dims):
    dot = functools.partial(
        lax.dot_general, dimension_numbers=(dims, ((), ())), preferred_element_type=jnp.float32
    )
    return dot(a_hi, b_hi) + dot(a_lo, b_hi) + dot(a_hi, b_lo)


def cos_turns(turns, period):
    v = (jnp.abs(turns.astype(jnp.float32) * (1.0 / period) - 0.5) - 0.25) * (2.0 * math.pi)
    v2 = v * v
    total = jnp.full_like(v, 1.0 / math.factorial(13))
    for order in (11, 9, 7, 5, 3, 1):
        sign = 1.0 if order % 4 == 1 else -1.0
        total = total * v2 + sign / math.factorial(order)
    return total * v


def rotation(turns, period):
    return cos_turns(turns & (period - 1), period), cos_turns((turns + period // 4) & (period - 1), period)

def surfaces(
    raw, own_drop, ty_hbm, tx_hbm, held, coh,
    buf, infos, acc, got, ends, phases, turns, ty, txs, *rest,
    slabs, groups, own_bins, own_w
):
    a_hi, a_lo, w_hi, w_lo, spec_y, spec_x = rest[:6]
    line_sem, x_sem, y_sem, diag_sem, recv_sem, isend_sem, irecv_sem, swap_sem, load_sem = rest[6:]
    slab, grp = lax.axis_index("slab"), lax.axis_index("grp")
    bits = slabs.bit_length() - 1
    line = slabs // 4
    rows = Q // 2
    bins = 2 * own_bins
    pairs = bins // 2
    cut = min(4, own_bins)
    cuts = own_bins // cut
    period = Q * HOP
    last = groups - 1
    zero = slab * 0
    core = slab % 2
    chip = (slab // 2) % 2
    level = slab // 4
    partner = (slab + 1 - 2 * core, grp)
    beside = (slab + 2 - 4 * chip, grp)
    across = (slab, 1 - grp)

    place = slab // 2

    def load(src, dst, i):
        return pltpu.make_async_copy(src, dst, load_sem.at[i])

    tables = [load(ty_hbm, ty, 0), load(tx_hbm.at[grp], txs, 1)]
    for copy in tables:
        copy.start()

    def chip_at(p):
        return (2 * p + core, grp)

    barrier = pltpu.get_barrier_semaphore()

    def greet(target):
        pl.semaphore_signal(barrier, inc=1, device_id=target, device_id_type=pl.DeviceIdType.MESH)

    def others(act):
        def body(i, carry):
            act((place + i) % (slabs // 2), i)
            return carry

        lax.fori_loop(1, slabs // 2, body, 0)

    greet(partner)
    greet(across)
    others(lambda p, i: greet(chip_at(p)))

    def at_step(i):
        return jnp.where(i <= level, level - i, i)

    def remote(src, dst, send, recv, target):
        return pltpu.make_async_remote_copy(
            src_ref=src, dst_ref=dst, send_sem=send, recv_sem=recv,
            device_id=target, device_id_type=pl.DeviceIdType.MESH,
        )

    def moved(z, dx, dg, send, target):
        at = 2 * z + (chip + dx) % 2
        g = (grp + dg) % groups
        return remote(buf.at[at, g], buf.at[at, g], send, recv_sem.at[at, g], target)

    def arrived(z, dx, dg):
        moved(z, dx, dg, line_sem.at[0], partner).wait_recv()

    def info_copy(first, count, send, recv, target):
        piece = infos.at[pl.ds(first, count)]
        return remote(piece, piece, isend_sem.at[send], irecv_sem.at[recv], target)

    chips = slabs // 2
    to_group = info_copy(slab, 1, 0, 0, across)
    to_partner = info_copy(slab, 1, chips, 1, partner)

    def to_chip(p, i):
        return info_copy(2 * place, 2, i, 2 + place, chip_at(p))

    def info_arrived(p):
        info_copy(2 * p, 2, 0, 2 + p, partner).wait_recv()

    def line_copy(z):
        return moved(level, 0, 0, line_sem.at[z], (slab + 4 * (z - level), grp))

    def lines(d):
        for z in (level - d, level + d):

            @pl.when((z >= 0) & (z < line))
            def _():
                line_copy(z).start()


    def to_x(i):
        return moved(at_step(i), 0, 0, x_sem.at[i], beside)

    def to_y(i):
        return moved(at_step(i), 0, 0, y_sem.at[i], across)

    def diagonal(i):
        odd = at_step(i) % 2
        return moved(at_step(i), odd, 1 - odd, diag_sem.at[i], (slab + (2 - 4 * chip) * (1 - odd), grp + odd * (1 - 2 * grp)))

    def from_line(i):
        arrived(at_step(i), 0, 0)
        to_x(i).start()
        to_y(i).start()

    def from_sides(i):
        odd = at_step(i) % 2
        arrived(at_step(i), odd, 1 - odd)
        diagonal(i).start()
        arrived(at_step(i), 1 - odd, odd)

    def run(first, end, act):
        def body(i, carry):
            act(i)
            return carry

        lax.fori_loop(first, end, body, 0)

    def reach(i):
        z = at_step(i)
        down = i <= level
        first = 2 * z - jnp.where(down & (z > 0), 1, 0)
        end = 2 * z + jnp.where(down & (i > 0), 1, 2)

        def wait(p):
            @pl.when(p != place)
            def _():
                info_arrived(p)

        run(first, end, wait)
        before = jnp.where(down, z + 1, z - 1)
        summed = jnp.where(down, z + 1, z)
        total = jnp.zeros((4, LANES), jnp.float32)
        for k in range(4):
            total = total + infos[4 * jnp.where(i == 0, z, summed) + k, 4:8, :] * jnp.where(
                (i > 0) | (4 * z + k > slab - core), 1.0, 0.0
            )
        base = ends[jnp.where(i == 0, z, before)] * jnp.where(i == 0, 0.0, 1.0)
        ends[z] = base + jnp.concatenate([total, total], axis=0) * jnp.where(down & (i > 0), -1.0, 1.0)

    for c in range(2):
        buf[place, grp, c * rows : (c + 1) * rows, :] = raw[:, c, :]

    @pl.when(grp == last)
    def _():
        infos[slab] = jnp.concatenate(
            [
                raw[rows - 2 :, 0, :],
                raw[rows - 2 :, 1, :],
                jnp.broadcast_to(own_drop[0].astype(jnp.float32), (4, LANES)),
            ],
            axis=0,
        )

    pl.semaphore_wait(barrier, chips + 1)

    @pl.when(grp == last)
    def _():
        to_group.start()
        to_partner.start()

    to_x(0).start()
    to_y(0).start()
    run(1, line, lines)
    ends[...] = jnp.zeros_like(ends)
    acc[...] = jnp.zeros_like(acc)

    lane = lax.broadcasted_iota(jnp.int32, (rows, LANES), 1)
    low = lane < HOP
    jlane = lax.broadcasted_iota(jnp.int32, (16, Q), 1)
    jlane = 2 * (jlane & (rows - 1)) + (jlane >= rows).astype(jnp.int32)
    turn = lax.broadcasted_iota(jnp.int32, (16, Q), 0)
    turn = jnp.where(turn < 8, 2 * turn + 1, 2 * bins * (slab // 2) + bins - 1)
    lanes8 = lax.broadcasted_iota(jnp.int32, (8, LANES), 1)
    lchan = KW + lanes8
    kchan = grp * own_w + (lanes8 & (own_w - 1))
    ksign = jnp.where(lanes8 < own_w, -1.0, 1.0)
    jsub = 2 * lax.broadcasted_iota(jnp.int32, (8, LANES), 0)

    def spread(array, count):
        return jnp.concatenate([array] * count, axis=0)

    def events(i, w, end=False):
        if end and w == 0:
            arrived(at_step(i), 1, 1)
        elif w == 0:
            from_sides(i + 1)
            reach(i + 1)
        elif w == 2:
            arrived(at_step(i), 1, 1)
        elif w == 3:

            @pl.when(i + 3 < line)
            def _():
                from_line(i + 3)

    def locate(u):
        h = u // 2
        far = ((h % 2 == 0) & (h > 0)) | (h == 2 * line - 1)
        i = jnp.where(far, (h - 1) // 2, (h + 1) // 2)
        z = at_step(i)
        n = 4 * z + 2 * ((chip + far.astype(jnp.int32)) % 2) + core
        return z, n, n // 2, 1 - u % 2

    def analyze(u, slot, first=False):
        z, n, at, g = locate(u)
        before = jnp.maximum(n - 1, 0)
        from_info = jnp.where((g == 0) & (n > 0), 1.0, 0.0)
        from_blk = jnp.where(g == 0, 0.0, 1.0)
        even, odd = [], []
        for c in range(2):
            base = c * rows
            tail = buf[at, 0, base + rows - 2 : base + rows, :]
            if not first:
                tail = tail * from_blk + infos[before, 2 * c : 2 * c + 2, :] * from_info
            r0 = buf[at, g, base : base + rows, :]
            r1 = jnp.concatenate([tail[1:2], buf[at, g, base : base + rows - 1, :]], axis=0)
            r2 = jnp.concatenate([tail, buf[at, g, base : base + rows - 2, :]], axis=0)
            even += [
                pltpu.roll(jnp.where(low, r1, r2), HOP, 1),
                pltpu.roll(jnp.where(low, r0, r1), HOP, 1),
            ]
            odd += [r1, r0]
        f_hi, f_lo = [], []
        for part in (even, odd):
            hi, lo = split(jnp.concatenate(part, axis=1))
            f_hi.append(hi)
            f_lo.append(lo)
        f_hi = jnp.concatenate(f_hi, axis=0)
        f_lo = jnp.concatenate(f_lo, axis=0)
        dot = functools.partial(jnp.dot, preferred_element_type=jnp.float32)
        upper = dot3(f_hi, f_lo, ty[0], ty[1], ((1,), (0,)))

        spec_y[slot] = upper

        def finish():
            twice = dot(f_hi, txs[...])
            spec_x[slot] = twice[:, :LANES] + dot(f_lo, txs[:, :LANES]) + twice[:, LANES:]

        return finish

    def build(u, slot, fresh, first=False):
        z, n, at, g = locate(u)
        if fresh:
            if first:
                rel = infos[slab, 4:8, :] * jnp.where(core > 0, 1.0, 0.0)
                rel = jnp.concatenate([rel, rel], axis=0)
            else:
                rel = ends[z]
                for k in range(1, 4):
                    drop = infos[4 * z + k, 4:8, :] * jnp.where(4 * z + k > n, 1.0, 0.0)
                    rel = rel - jnp.concatenate([drop, drop], axis=0)
            stamp = rel.astype(jnp.int32)
            t = (spread(stamp, 2) + HOP * jlane) & (period - 1)
            phq = rotation((turn * t) & (2 * period - 1), 2 * period)
            phx = [rotation(kchan * ((stamp + HOP * (jsub + p)) & (NCH - 1)), NCH) for p in range(2)]
            phy = [rotation(lchan * ((stamp + HOP * (jsub + p)) & (NCH - 1)), NCH) for p in range(2)]
            for p in range(2):
                for k in range(2):
                    phases[4 * p + k] = phx[p][k] * (ksign if k else 1.0)
                    phases[4 * p + 2 + k] = phy[p][k]
            turns[0] = phq[0]
            turns[1] = phq[1]
        phx = [(phases[4 * p], phases[4 * p + 1]) for p in range(2)]
        phy = [(phases[4 * p + 2], phases[4 * p + 3]) for p in range(2)]
        phq = turns[0], turns[1]
        zrs, zis, kxs = [], [], []
        for p in range(2):
            c, s = (spread(v, rows // 8) for v in phy[p])
            part = spec_y[slot, p * rows : (p + 1) * rows, :]
            yr, yi = part[:, :LW], part[:, LW:]
            zrs.append(yr * c - yi * s)
            zis.append(yr * s + yi * c)
            c, s = spread(phx[p][0], rows // 8), spread(phx[p][1], rows // 8)
            part = spec_x[slot, p * rows : (p + 1) * rows, :]
            kxs.append(part * c + pltpu.roll(part, own_w, 1) * s)
        zr_hi, zr_lo = split(jnp.concatenate(zrs, axis=0))
        zi_hi, zi_lo = split(jnp.concatenate(zis, axis=0))

        def weights(zr, zi):
            return jnp.concatenate(
                [jnp.concatenate([zr, -zi], 1), jnp.concatenate([zi, zr], 1)], axis=0
            )

        w_hi[slot] = weights(zr_hi, zi_hi)
        w_lo[slot] = weights(zr_lo, zi_lo)
        x = jnp.concatenate(kxs, axis=0).T
        xr, xi = x[:own_w], x[own_w:]
        c, s = phq[0][8:9], phq[1][8:9]
        ur = xr * c - xi * s
        ui = xr * s + xi * c

        def put(q, real, imag):
            hi, lo = split(jnp.concatenate([real, imag], axis=1))
            a_hi[slot, q * own_w : (q + 1) * own_w, :] = hi
            a_lo[slot, q * own_w : (q + 1) * own_w, :] = lo

        def turned(c):
            for m in range(c * cut // 2, (c + 1) * cut // 2):
                c, s = phq[0][m : m + 1], phq[1][m : m + 1]
                rc, rs, ic, is_ = ur * c, ur * s, ui * c, ui * s
                put(pairs + m, rc - is_, ic + rs)
                put(pairs - 1 - m, rc + is_, ic - rs)

        return turned

    def accumulate(slot, c, late):
        count = cut * own_w
        at = pl.ds(c * count if isinstance(c, int) else pl.multiple_of(c * count, count), count)
        hi = a_hi[slot, at, :]
        dot = functools.partial(jnp.dot, preferred_element_type=jnp.float32)
        both = jnp.concatenate([hi, a_lo[slot, at, :]], axis=0)
        if late:
            once = dot(hi, w_lo[slot])
            twice = dot(both, w_hi[slot])
        else:
            twice = dot(both, w_hi[slot])
            once = dot(hi, w_lo[slot])
        part = twice[:count] + twice[count:] + once
        sr = part[:, :LW].reshape(cut, own_w, LW)
        si = part[:, LW:].reshape(cut, own_w, LW)
        half, piece = c // cuts, c % cuts
        q = pl.ds(piece * cut, cut)
        acc[half, 0, q] = jnp.maximum(acc[half, 0, q], sr * sr + si * si)
        acc[half, 1, q] = acc[half, 1, q] + sr
        acc[half, 2, q] = acc[half, 2, q] + si

    units = 4 * line

    def step(i, w, slot, end=False):
        u = 4 * i + w
        slot = u % 2
        events(i, w, end)
        accumulate(slot, 0, 0)
        turned = build(u + 1, 1 - slot, w % 2 == 1)
        finish = analyze(u + 2, slot)
        turned(0)
        for c in range(1, 2 * cuts):
            accumulate(slot, c, c % 2)
            if c == 1:
                finish()
            turned(c)
        return 1 - slot

    def steps(i, slot):
        for w in range(4):
            slot = step(i, w, slot)
        return slot

    if line > 1:
        from_line(zero + 1)
    from_sides(zero)
    for copy in tables:
        copy.wait()
    analyze(zero, 0, True)()

    @pl.when(grp != last)
    def _():
        to_group.wait_recv()
        to_partner.start()

    info_copy(slab + 1 - 2 * core, 1, 0, 1, partner).wait_recv()
    others(lambda p, i: to_chip(p, i).start())
    if line > 2:
        from_line(zero + 2)
    reach(zero)
    turned = build(zero, 0, True, True)
    analyze(zero + 1, 1)()
    for c in range(2 * cuts):
        turned(c)
    slot = lax.fori_loop(0, line - 1, steps, zero)
    slot = step(zero + line - 1, 0, slot, True)
    step(zero + line - 1, 1, slot, True)
    slot = 0
    turned = build(zero + units - 1, 1 - slot, False)
    for c in range(2 * cuts):
        turned(c)
    def swap(c):
        q = pl.ds(c * cut, cut)
        return [
            remote(
                acc.at[1 - core, k, q], got.at[k, q], swap_sem.at[0, 3 * c + k], swap_sem.at[1, 3 * c + k], partner
            )
            for k in range(3)
        ]

    for c in range(cuts):
        for late, other in enumerate((slot, 1 - slot)):
            accumulate(other, (1 - core) * cuts + c, late)
        for copy in swap(c):
            copy.start()
    for c in range(cuts):
        for late, other in enumerate((slot, 1 - slot)):
            accumulate(other, core * cuts + c, late)

    total = jnp.zeros((4, LANES), jnp.float32)
    for k in range(4):
        total = total + infos[k, 4:8, :]
    stamp = (jnp.concatenate([total, total], axis=0) - ends[0]).astype(jnp.int32) & (period - 1)
    klane = lax.broadcasted_iota(jnp.int32, (own_w, LANES), 1)
    ksub = grp * own_w + lax.broadcasted_iota(jnp.int32, (own_w, LANES), 0)
    kl = rotation((ksub - KW - klane) * spread(stamp, own_w // 8), NCH)
    qrow = slab * own_bins + lax.broadcasted_iota(jnp.int32, (8, LANES), 0)
    ql = rotation(qrow * stamp, period)
    scale = 1.0 / math.sqrt(slabs * BLOCKS)
    for c in range(cuts):
        for copy in swap(c):
            copy.wait_recv()
    held[...] = jnp.sqrt(jnp.maximum(acc[core, 0], got[0]))
    for q in range(own_bins):
        c, s = ql[0][q : q + 1] * scale, ql[1][q : q + 1] * scale
        fc = kl[0] * c - kl[1] * s
        fs = kl[0] * s + kl[1] * c
        real = acc[core, 1, q] + got[1, q]
        imag = acc[core, 2, q] + got[2, q]
        coh[0, q] = real * fc - imag * fs
        coh[1, q] = real * fs + imag * fc

    @pl.when(grp == last)
    def _():
        to_group.wait_send()

    to_partner.wait_send()
    others(lambda p, i: to_chip(p, i).wait_send())
    run(1, line, lambda i: line_copy((level + i) % line).wait_send())

    def sent(i):
        to_x(i).wait_send()
        to_y(i).wait_send()
        diagonal(i).wait_send()

    run(0, line, sent)
    for c in range(cuts):
        for copy in swap(c):
            copy.wait_send()


def put_out(held, coh, held_out, coh_out, sems):
    copies = [
        pltpu.make_async_copy(held, held_out, sems.at[0]),
        pltpu.make_async_copy(coh, coh_out, sems.at[1]),
    ]
    for copy in copies:
        copy.start()
    for copy in copies:
        copy.wait()


def on_device(capture, dropped):
    slabs = lax.axis_size("slab")
    groups = lax.axis_size("grp")
    own_bins = Q // slabs
    own_w = KW // groups
    local = capture.shape[1] // LANES
    to_real, to_imag = dft_tables()
    ty = np.concatenate([to_real[:, KW:], to_imag[:, KW:]], 1)
    tx = np.stack(
        [
            np.concatenate(
                [to_real[:, g * own_w : (g + 1) * own_w], to_imag[:, g * own_w : (g + 1) * own_w]], 1
            )
            for g in range(groups)
        ]
    ) / math.sqrt(Q)
    ty = jnp.stack(split_np(ty))
    txs = jnp.concatenate(split_np(tx), axis=2)
    blocks = capture.reshape(2, local, LANES).transpose(1, 0, 2)
    dma = pltpu.SemaphoreType.DMA
    line = slabs // 4
    count = 2 * own_bins * own_w
    slot = [pltpu.VMEM((2, count, 2 * Q), jnp.bfloat16)] * 2
    slot = slot + [pltpu.VMEM((2, 2 * Q, 2 * LW), jnp.bfloat16)] * 2
    slot = slot + [pltpu.VMEM((2, Q, w), jnp.float32) for w in (2 * LW, LANES)]
    results = pl.pallas_call(
        functools.partial(surfaces, slabs=slabs, groups=groups, own_bins=own_bins, own_w=own_w),
        out_shape=[
            jax.ShapeDtypeStruct((own_bins, own_w, LW), jnp.float32),
            jax.ShapeDtypeStruct((2, own_bins, own_w, LW), jnp.float32),
        ],
        in_specs=[pl.BlockSpec(memory_space=space) for space in (pltpu.VMEM, pltpu.SMEM, pltpu.HBM, pltpu.HBM)],
        out_specs=[pl.BlockSpec(memory_space=pltpu.VMEM)] * 2,
        scratch_shapes=[
            pltpu.VMEM((slabs // 2, groups, 2 * local, LANES), jnp.float32),
            pltpu.VMEM((slabs, 8, LANES), jnp.float32),
            pltpu.VMEM((2, 3, own_bins, own_w, LW), jnp.float32),
            pltpu.VMEM((3, own_bins, own_w, LW), jnp.float32),
            pltpu.VMEM((line, 8, LANES), jnp.float32),
            pltpu.VMEM((8, 8, LANES), jnp.float32),
            pltpu.VMEM((2, 16, LANES), jnp.float32),
            pltpu.VMEM(ty.shape, jnp.bfloat16),
            pltpu.VMEM(txs.shape[1:], jnp.bfloat16),
            *slot,
            dma((line,)),
            dma((line,)),
            dma((line,)),
            dma((line,)),
            dma((slabs // 2, groups)),
            dma((slabs // 2 + 1,)),
            dma((slabs // 2 + 2,)),
            dma((2, 3 * own_bins)),
            dma((2,)),
        ],
        compiler_params=pltpu.CompilerParams(
            collective_id=0, has_side_effects=True, vmem_limit_bytes=VMEM_LIMIT
        ),
    )(
        blocks,
        dropped,
        ty,
        txs,
    )
    return pl.pallas_call(
        put_out,
        out_shape=[jax.ShapeDtypeStruct(r.shape, r.dtype) for r in results],
        in_specs=[pl.BlockSpec(memory_space=pltpu.VMEM)] * 2,
        out_specs=[pl.BlockSpec(memory_space=pltpu.HBM)] * 2,
        scratch_shapes=[dma((2,))],
        compiler_params=pltpu.CompilerParams(vmem_limit_bytes=2**20),
    )(*results)


def solution(mesh):
    in_specs = (P(None, ("slab", "grp")), P("slab"))
    out_specs = (P("slab", "grp", None), P(None, "slab", "grp", None))
    return jax.shard_map(
        on_device, mesh=mesh, in_specs=in_specs, out_specs=out_specs, check_vma=False
    )
```

```python
import functools
import math

import jax
import jax.numpy as jnp
import numpy as np
from jax import lax
from jax.experimental import pallas as pl
from jax.experimental.pallas import tpu as pltpu
from jax.sharding import PartitionSpec as P

NCH = 256
HOP = 64
KW = 128
LW = 128
Q = 128
BLOCKS = 2
LANES = 128
VMEM_LIMIT = 67043328 - 11300 * 2**10


def split_np(table):
    hi = table.astype(jnp.bfloat16)
    lo = (table - hi.astype(np.float64)).astype(jnp.bfloat16)
    return jnp.asarray(hi), jnp.asarray(lo)


def split(values):
    hi = values.astype(jnp.bfloat16)
    lo = (values - hi.astype(jnp.float32)).astype(jnp.bfloat16)
    return hi, lo


def dft_tables():
    i = np.arange(NCH)
    w = 0.5 - 0.5 * np.cos(2.0 * np.pi * i / NCH)
    w = w / np.sqrt(np.sum(w * w))
    turns = (i[:, None] * i[None, :] % NCH) * (2.0 * np.pi / NCH)
    cos, sin = w[:, None] * np.cos(turns), w[:, None] * np.sin(turns)
    to_real = np.concatenate([cos, sin], 0)
    to_imag = np.concatenate([-sin, cos], 0)
    return to_real, to_imag


def dot3(a_hi, a_lo, b_hi, b_lo, dims):
    dot = functools.partial(
        lax.dot_general, dimension_numbers=(dims, ((), ())), preferred_element_type=jnp.float32
    )
    return dot(a_hi, b_hi) + dot(a_lo, b_hi) + dot(a_hi, b_lo)


def cos_turns(turns, period):
    v = (jnp.abs(turns.astype(jnp.float32) * (1.0 / period) - 0.5) - 0.25) * (2.0 * math.pi)
    v2 = v * v
    total = jnp.full_like(v, 1.0 / math.factorial(13))
    for order in (11, 9, 7, 5, 3, 1):
        sign = 1.0 if order % 4 == 1 else -1.0
        total = total * v2 + sign / math.factorial(order)
    return total * v


def rotation(turns, period):
    return cos_turns(turns & (period - 1), period), cos_turns((turns + period // 4) & (period - 1), period)

def surfaces(
    raw, own_drop, ty_hbm, tx_hbm, held, coh,
    buf, infos, acc, got, ends, phases, turns, ty, txs, *rest,
    slabs, groups, own_bins, own_w
):
    a_hi, a_lo, w_hi, w_lo, spec_y, spec_x = rest[:6]
    line_sem, x_sem, y_sem, diag_sem, recv_sem, isend_sem, irecv_sem, swap_sem, load_sem = rest[6:]
    slab, grp = lax.axis_index("slab"), lax.axis_index("grp")
    bits = slabs.bit_length() - 1
    line = slabs // 4
    rows = Q // 2
    bins = 2 * own_bins
    pairs = bins // 2
    cut = min(4, own_bins)
    cuts = own_bins // cut
    period = Q * HOP
    last = groups - 1
    zero = slab * 0
    core = slab % 2
    chip = (slab // 2) % 2
    level = slab // 4
    partner = (slab + 1 - 2 * core, grp)
    beside = (slab + 2 - 4 * chip, grp)
    across = (slab, 1 - grp)

    place = slab // 2

    def load(src, dst, i):
        return pltpu.make_async_copy(src, dst, load_sem.at[i])

    tables = [load(ty_hbm, ty, 0), load(tx_hbm.at[grp], txs, 1)]
    for copy in tables:
        copy.start()

    def chip_at(p):
        return (2 * p + core, grp)

    barrier = pltpu.get_barrier_semaphore()

    def greet(target):
        pl.semaphore_signal(barrier, inc=1, device_id=target, device_id_type=pl.DeviceIdType.MESH)

    def others(act):
        def body(i, carry):
            act((place + i) % (slabs // 2), i)
            return carry

        lax.fori_loop(1, slabs // 2, body, 0)

    greet(partner)
    greet(across)
    others(lambda p, i: greet(chip_at(p)))

    def at_step(i):
        return jnp.where(i <= level, level - i, i)

    def remote(src, dst, send, recv, target):
        return pltpu.make_async_remote_copy(
            src_ref=src, dst_ref=dst, send_sem=send, recv_sem=recv,
            device_id=target, device_id_type=pl.DeviceIdType.MESH,
        )

    def moved(z, dx, dg, send, target):
        at = 2 * z + (chip + dx) % 2
        g = (grp + dg) % groups
        return remote(buf.at[at, g], buf.at[at, g], send, recv_sem.at[at, g], target)

    def arrived(z, dx, dg):
        moved(z, dx, dg, line_sem.at[0], partner).wait_recv()

    def info_copy(first, count, send, recv, target):
        piece = infos.at[pl.ds(first, count)]
        return remote(piece, piece, isend_sem.at[send], irecv_sem.at[recv], target)

    chips = slabs // 2
    to_group = info_copy(slab, 1, 0, 0, across)
    to_partner = info_copy(slab, 1, chips, 1, partner)

    def to_chip(p, i):
        return info_copy(2 * place, 2, i, 2 + place, chip_at(p))

    def info_arrived(p):
        info_copy(2 * p, 2, 0, 2 + p, partner).wait_recv()

    def line_copy(z):
        return moved(level, 0, 0, line_sem.at[z], (slab + 4 * (z - level), grp))

    def lines(d):
        for z in (level - d, level + d):

            @pl.when((z >= 0) & (z < line))
            def _():
                line_copy(z).start()


    def to_x(i):
        return moved(at_step(i), 0, 0, x_sem.at[i], beside)

    def to_y(i):
        return moved(at_step(i), 0, 0, y_sem.at[i], across)

    def diagonal(i):
        odd = at_step(i) % 2
        return moved(at_step(i), odd, 1 - odd, diag_sem.at[i], (slab + (2 - 4 * chip) * (1 - odd), grp + odd * (1 - 2 * grp)))

    def from_line(i):
        arrived(at_step(i), 0, 0)
        to_x(i).start()
        to_y(i).start()

    def from_sides(i):
        odd = at_step(i) % 2
        arrived(at_step(i), odd, 1 - odd)
        diagonal(i).start()
        arrived(at_step(i), 1 - odd, odd)

    def run(first, end, act):
        def body(i, carry):
            act(i)
            return carry

        lax.fori_loop(first, end, body, 0)

    def reach(i):
        z = at_step(i)
        down = i <= level
        first = 2 * z - jnp.where(down & (z > 0), 1, 0)
        end = 2 * z + jnp.where(down & (i > 0), 1, 2)

        def wait(p):
            @pl.when(p != place)
            def _():
                info_arrived(p)

        run(first, end, wait)
        before = jnp.where(down, z + 1, z - 1)
        summed = jnp.where(down, z + 1, z)
        total = jnp.zeros((4, LANES), jnp.float32)
        for k in range(4):
            total = total + infos[4 * jnp.where(i == 0, z, summed) + k, 4:8, :] * jnp.where(
                (i > 0) | (4 * z + k > slab - core), 1.0, 0.0
            )
        base = ends[jnp.where(i == 0, z, before)] * jnp.where(i == 0, 0.0, 1.0)
        ends[z] = base + jnp.concatenate([total, total], axis=0) * jnp.where(down & (i > 0), -1.0, 1.0)

    for c in range(2):
        buf[place, grp, c * rows : (c + 1) * rows, :] = raw[:, c, :]

    @pl.when(grp == last)
    def _():
        infos[slab] = jnp.concatenate(
            [
                raw[rows - 2 :, 0, :],
                raw[rows - 2 :, 1, :],
                jnp.broadcast_to(own_drop[0].astype(jnp.float32), (4, LANES)),
            ],
            axis=0,
        )

    pl.semaphore_wait(barrier, chips + 1)

    @pl.when(grp == last)
    def _():
        to_group.start()
        to_partner.start()

    to_x(0).start()
    to_y(0).start()
    run(1, line, lines)
    ends[...] = jnp.zeros_like(ends)
    acc[...] = jnp.zeros_like(acc)

    lane = lax.broadcasted_iota(jnp.int32, (rows, LANES), 1)
    low = lane < HOP
    jlane = lax.broadcasted_iota(jnp.int32, (16, Q), 1)
    jlane = 2 * (jlane & (rows - 1)) + (jlane >= rows).astype(jnp.int32)
    turn = lax.broadcasted_iota(jnp.int32, (16, Q), 0)
    turn = jnp.where(turn < 8, 2 * turn + 1, 2 * bins * (slab // 2) + bins - 1)
    lanes8 = lax.broadcasted_iota(jnp.int32, (8, LANES), 1)
    lchan = KW + lanes8
    kchan = grp * own_w + (lanes8 & (own_w - 1))
    ksign = jnp.where(lanes8 < own_w, -1.0, 1.0)
    jsub = 2 * lax.broadcasted_iota(jnp.int32, (8, LANES), 0)

    def spread(array, count):
        return jnp.concatenate([array] * count, axis=0)

    def events(i, w, end=False):
        if end and w == 0:
            arrived(at_step(i), 1, 1)
        elif w == 0:
            from_sides(i + 1)
            reach(i + 1)
        elif w == 2:
            arrived(at_step(i), 1, 1)
        elif w == 3:

            @pl.when(i + 3 < line)
            def _():
                from_line(i + 3)

    def locate(u):
        h = u // 2
        far = ((h % 2 == 0) & (h > 0)) | (h == 2 * line - 1)
        i = jnp.where(far, (h - 1) // 2, (h + 1) // 2)
        z = at_step(i)
        n = 4 * z + 2 * ((chip + far.astype(jnp.int32)) % 2) + core
        return z, n, n // 2, 1 - u % 2

    def analyze(u, slot, first=False):
        z, n, at, g = locate(u)
        before = jnp.maximum(n - 1, 0)
        from_info = jnp.where((g == 0) & (n > 0), 1.0, 0.0)
        from_blk = jnp.where(g == 0, 0.0, 1.0)
        even, odd = [], []
        for c in range(2):
            base = c * rows
            tail = buf[at, 0, base + rows - 2 : base + rows, :]
            if not first:
                tail = tail * from_blk + infos[before, 2 * c : 2 * c + 2, :] * from_info
            r0 = buf[at, g, base : base + rows, :]
            r1 = jnp.concatenate([tail[1:2], buf[at, g, base : base + rows - 1, :]], axis=0)
            r2 = jnp.concatenate([tail, buf[at, g, base : base + rows - 2, :]], axis=0)
            even += [
                pltpu.roll(jnp.where(low, r1, r2), HOP, 1),
                pltpu.roll(jnp.where(low, r0, r1), HOP, 1),
            ]
            odd += [r1, r0]
        f_hi, f_lo = [], []
        for part in (even, odd):
            hi, lo = split(jnp.concatenate(part, axis=1))
            f_hi.append(hi)
            f_lo.append(lo)
        f_hi = jnp.concatenate(f_hi, axis=0)
        f_lo = jnp.concatenate(f_lo, axis=0)
        dot = functools.partial(jnp.dot, preferred_element_type=jnp.float32)
        upper = dot3(f_hi, f_lo, ty[0], ty[1], ((1,), (0,)))

        spec_y[slot] = upper

        def finish():
            twice = dot(f_hi, txs[...])
            spec_x[slot] = twice[:, :LANES] + dot(f_lo, txs[:, :LANES]) + twice[:, LANES:]

        return finish

    def build(u, slot, fresh, first=False):
        z, n, at, g = locate(u)
        if fresh:
            if first:
                rel = infos[slab, 4:8, :] * jnp.where(core > 0, 1.0, 0.0)
                rel = jnp.concatenate([rel, rel], axis=0)
            else:
                rel = ends[z]
                for k in range(1, 4):
                    drop = infos[4 * z + k, 4:8, :] * jnp.where(4 * z + k > n, 1.0, 0.0)
                    rel = rel - jnp.concatenate([drop, drop], axis=0)
            stamp = rel.astype(jnp.int32)
            t = (spread(stamp, 2) + HOP * jlane) & (period - 1)
            phq = rotation((turn * t) & (2 * period - 1), 2 * period)
            phx = [rotation(kchan * ((stamp + HOP * (jsub + p)) & (NCH - 1)), NCH) for p in range(2)]
            phy = [rotation(lchan * ((stamp + HOP * (jsub + p)) & (NCH - 1)), NCH) for p in range(2)]
            for p in range(2):
                for k in range(2):
                    phases[4 * p + k] = phx[p][k] * (ksign if k else 1.0)
                    phases[4 * p + 2 + k] = phy[p][k]
            turns[0] = phq[0]
            turns[1] = phq[1]
        phx = [(phases[4 * p], phases[4 * p + 1]) for p in range(2)]
        phy = [(phases[4 * p + 2], phases[4 * p + 3]) for p in range(2)]
        phq = turns[0], turns[1]
        zrs, zis, kxs = [], [], []
        for p in range(2):
            c, s = (spread(v, rows // 8) for v in phy[p])
            part = spec_y[slot, p * rows : (p + 1) * rows, :]
            yr, yi = part[:, :LW], part[:, LW:]
            zrs.append(yr * c - yi * s)
            zis.append(yr * s + yi * c)
            c, s = spread(phx[p][0], rows // 8), spread(phx[p][1], rows // 8)
            part = spec_x[slot, p * rows : (p + 1) * rows, :]
            kxs.append(part * c + pltpu.roll(part, own_w, 1) * s)
        zr_hi, zr_lo = split(jnp.concatenate(zrs, axis=0))
        zi_hi, zi_lo = split(jnp.concatenate(zis, axis=0))

        def weights(zr, zi):
            return jnp.concatenate(
                [jnp.concatenate([zr, -zi], 1), jnp.concatenate([zi, zr], 1)], axis=0
            )

        w_hi[slot] = weights(zr_hi, zi_hi)
        w_lo[slot] = weights(zr_lo, zi_lo)
        x = jnp.concatenate(kxs, axis=0).T
        xr, xi = x[:own_w], x[own_w:]
        c, s = phq[0][8:9], phq[1][8:9]
        ur = xr * c - xi * s
        ui = xr * s + xi * c

        def put(q, real, imag):
            hi, lo = split(jnp.concatenate([real, imag], axis=1))
            a_hi[slot, q * own_w : (q + 1) * own_w, :] = hi
            a_lo[slot, q * own_w : (q + 1) * own_w, :] = lo

        def turned(c):
            for m in range(c * cut // 2, (c + 1) * cut // 2):
                c, s = phq[0][m : m + 1], phq[1][m : m + 1]
                rc, rs, ic, is_ = ur * c, ur * s, ui * c, ui * s
                put(pairs + m, rc - is_, ic + rs)
                put(pairs - 1 - m, rc + is_, ic - rs)

        return turned

    def accumulate(slot, c, late):
        count = cut * own_w
        at = pl.ds(c * count if isinstance(c, int) else pl.multiple_of(c * count, count), count)
        hi = a_hi[slot, at, :]
        dot = functools.partial(jnp.dot, preferred_element_type=jnp.float32)
        both = jnp.concatenate([hi, a_lo[slot, at, :]], axis=0)
        if late:
            once = dot(hi, w_lo[slot])
            twice = dot(both, w_hi[slot])
        else:
            twice = dot(both, w_hi[slot])
            once = dot(hi, w_lo[slot])
        part = twice[:count] + twice[count:] + once
        sr = part[:, :LW].reshape(cut, own_w, LW)
        si = part[:, LW:].reshape(cut, own_w, LW)
        half, piece = c // cuts, c % cuts
        q = pl.ds(piece * cut, cut)
        acc[half, 0, q] = jnp.maximum(acc[half, 0, q], sr * sr + si * si)
        acc[half, 1, q] = acc[half, 1, q] + sr
        acc[half, 2, q] = acc[half, 2, q] + si

    units = 4 * line

    def step(i, w, slot, end=False):
        u = 4 * i + w
        slot = u % 2
        events(i, w, end)
        accumulate(slot, 0, 0)
        turned = build(u + 1, 1 - slot, w % 2 == 1)
        finish = analyze(u + 2, slot)
        turned(0)
        for c in range(1, 2 * cuts):
            accumulate(slot, c, c % 2)
            if c == 1:
                finish()
            turned(c)
        return 1 - slot

    def steps(i, slot):
        for w in range(4):
            slot = step(i, w, slot)
        return slot

    @pl.when(grp != last)
    def _():
        to_group.wait_recv()
        to_partner.start()

    if line > 1:
        from_line(zero + 1)
    from_sides(zero)
    for copy in tables:
        copy.wait()
    analyze(zero, 0, True)()

    info_copy(slab + 1 - 2 * core, 1, 0, 1, partner).wait_recv()
    others(lambda p, i: to_chip(p, i).start())
    if line > 2:
        from_line(zero + 2)
    reach(zero)
    turned = build(zero, 0, True, True)
    analyze(zero + 1, 1)()
    for c in range(2 * cuts):
        turned(c)
    slot = lax.fori_loop(0, line - 1, steps, zero)
    slot = step(zero + line - 1, 0, slot, True)
    step(zero + line - 1, 1, slot, True)
    slot = 0
    turned = build(zero + units - 1, 1 - slot, False)
    for c in range(2 * cuts):
        turned(c)
    def swap(c):
        q = pl.ds(c * cut, cut)
        return [
            remote(
                acc.at[1 - core, k, q], got.at[k, q], swap_sem.at[0, 3 * c + k], swap_sem.at[1, 3 * c + k], partner
            )
            for k in range(3)
        ]

    for c in range(cuts):
        for late, other in enumerate((slot, 1 - slot)):
            accumulate(other, (1 - core) * cuts + c, late)
        for copy in swap(c):
            copy.start()
    for c in range(cuts):
        for late, other in enumerate((slot, 1 - slot)):
            accumulate(other, core * cuts + c, late)

    total = jnp.zeros((4, LANES), jnp.float32)
    for k in range(4):
        total = total + infos[k, 4:8, :]
    stamp = (jnp.concatenate([total, total], axis=0) - ends[0]).astype(jnp.int32) & (period - 1)
    klane = lax.broadcasted_iota(jnp.int32, (own_w, LANES), 1)
    ksub = grp * own_w + lax.broadcasted_iota(jnp.int32, (own_w, LANES), 0)
    kl = rotation((ksub - KW - klane) * spread(stamp, own_w // 8), NCH)
    qrow = slab * own_bins + lax.broadcasted_iota(jnp.int32, (8, LANES), 0)
    ql = rotation(qrow * stamp, period)
    scale = 1.0 / math.sqrt(slabs * BLOCKS)
    for c in range(cuts):
        for copy in swap(c):
            copy.wait_recv()
    held[...] = jnp.sqrt(jnp.maximum(acc[core, 0], got[0]))
    for q in range(own_bins):
        c, s = ql[0][q : q + 1] * scale, ql[1][q : q + 1] * scale
        fc = kl[0] * c - kl[1] * s
        fs = kl[0] * s + kl[1] * c
        real = acc[core, 1, q] + got[1, q]
        imag = acc[core, 2, q] + got[2, q]
        coh[0, q] = real * fc - imag * fs
        coh[1, q] = real * fs + imag * fc

    @pl.when(grp == last)
    def _():
        to_group.wait_send()

    to_partner.wait_send()
    others(lambda p, i: to_chip(p, i).wait_send())
    run(1, line, lambda i: line_copy((level + i) % line).wait_send())

    def sent(i):
        to_x(i).wait_send()
        to_y(i).wait_send()
        diagonal(i).wait_send()

    run(0, line, sent)
    for c in range(cuts):
        for copy in swap(c):
            copy.wait_send()


def put_out(held, coh, held_out, coh_out, sems):
    copies = [
        pltpu.make_async_copy(held, held_out, sems.at[0]),
        pltpu.make_async_copy(coh, coh_out, sems.at[1]),
    ]
    for copy in copies:
        copy.start()
    for copy in copies:
        copy.wait()


def on_device(capture, dropped):
    slabs = lax.axis_size("slab")
    groups = lax.axis_size("grp")
    own_bins = Q // slabs
    own_w = KW // groups
    local = capture.shape[1] // LANES
    to_real, to_imag = dft_tables()
    ty = np.concatenate([to_real[:, KW:], to_imag[:, KW:]], 1)
    tx = np.stack(
        [
            np.concatenate(
                [to_real[:, g * own_w : (g + 1) * own_w], to_imag[:, g * own_w : (g + 1) * own_w]], 1
            )
            for g in range(groups)
        ]
    ) / math.sqrt(Q)
    ty = jnp.stack(split_np(ty))
    txs = jnp.concatenate(split_np(tx), axis=2)
    blocks = capture.reshape(2, local, LANES).transpose(1, 0, 2)
    dma = pltpu.SemaphoreType.DMA
    line = slabs // 4
    count = 2 * own_bins * own_w
    slot = [pltpu.VMEM((2, count, 2 * Q), jnp.bfloat16)] * 2
    slot = slot + [pltpu.VMEM((2, 2 * Q, 2 * LW), jnp.bfloat16)] * 2
    slot = slot + [pltpu.VMEM((2, Q, w), jnp.float32) for w in (2 * LW, LANES)]
    results = pl.pallas_call(
        functools.partial(surfaces, slabs=slabs, groups=groups, own_bins=own_bins, own_w=own_w),
        out_shape=[
            jax.ShapeDtypeStruct((own_bins, own_w, LW), jnp.float32),
            jax.ShapeDtypeStruct((2, own_bins, own_w, LW), jnp.float32),
        ],
        in_specs=[pl.BlockSpec(memory_space=space) for space in (pltpu.VMEM, pltpu.SMEM, pltpu.HBM, pltpu.HBM)],
        out_specs=[pl.BlockSpec(memory_space=pltpu.VMEM)] * 2,
        scratch_shapes=[
            pltpu.VMEM((slabs // 2, groups, 2 * local, LANES), jnp.float32),
            pltpu.VMEM((slabs, 8, LANES), jnp.float32),
            pltpu.VMEM((2, 3, own_bins, own_w, LW), jnp.float32),
            pltpu.VMEM((3, own_bins, own_w, LW), jnp.float32),
            pltpu.VMEM((line, 8, LANES), jnp.float32),
            pltpu.VMEM((8, 8, LANES), jnp.float32),
            pltpu.VMEM((2, 16, LANES), jnp.float32),
            pltpu.VMEM(ty.shape, jnp.bfloat16),
            pltpu.VMEM(txs.shape[1:], jnp.bfloat16),
            *slot,
            dma((line,)),
            dma((line,)),
            dma((line,)),
            dma((line,)),
            dma((slabs // 2, groups)),
            dma((slabs // 2 + 1,)),
            dma((slabs // 2 + 2,)),
            dma((2, 3 * own_bins)),
            dma((2,)),
        ],
        compiler_params=pltpu.CompilerParams(
            collective_id=0, has_side_effects=True, vmem_limit_bytes=VMEM_LIMIT
        ),
    )(
        blocks,
        dropped,
        ty,
        txs,
    )
    return pl.pallas_call(
        put_out,
        out_shape=[jax.ShapeDtypeStruct(r.shape, r.dtype) for r in results],
        in_specs=[pl.BlockSpec(memory_space=pltpu.VMEM)] * 2,
        out_specs=[pl.BlockSpec(memory_space=pltpu.HBM)] * 2,
        scratch_shapes=[dma((2,))],
        compiler_params=pltpu.CompilerParams(vmem_limit_bytes=2**20),
    )(*results)


def solution(mesh):
    in_specs = (P(None, ("slab", "grp")), P("slab"))
    out_specs = (P("slab", "grp", None), P(None, "slab", "grp", None))
    return jax.shard_map(
        on_device, mesh=mesh, in_specs=in_specs, out_specs=out_specs, check_vma=False
    )
```
